32 devices in a mesh: conv: 4 (over y, core), seq: 4 (over z), tensor: 2 (over x).
Axes of the slice: x: 2, y: 2, z: 4, core: 2. Of those that a mesh axis runs over, the one named last changes fastest.
Arguments:
- queries: bfloat16 [4, 512, 4096], P('conv', 'seq', 'tensor'), may hold values from -6 to 6
- keys: bfloat16 [8, 1664, 1024], P('conv', ('seq', 'tensor')), may hold values from -6 to 6
- values: bfloat16 [8, 1664, 1024], P('conv', ('seq', 'tensor')), may hold values from -18 to 18
- q_gain: float32 [128], replicated, may hold values from 0.9 to 2.2
- k_gain: float32 [128], replicated, may hold values from 0.9 to 2.2
- gate: float32 [1], replicated, may hold values from 0.4 to 1.6
- tile_count: int32 [4], replicated, may hold values from 1 to 2, as said below
- tile_owner: int32 [4, 2], replicated, may hold values from -1 to 3, as said below
- visible: int32 [4, 512], replicated, may hold values from 0 to 2, as said below
- d_out: bfloat16 [4, 512, 4096], P('conv', 'seq', 'tensor'), may hold values from -12 to 12
Outputs:
- attended: bfloat16 [4, 512, 4096], P('conv', 'seq', 'tensor')
- d_queries: bfloat16 [4, 512, 4096], P('conv', 'seq', 'tensor')
- d_keys: bfloat16 [8, 1664, 1024], P('conv', ('seq', 'tensor'))
- d_values: bfloat16 [8, 1664, 1024], P('conv', ('seq', 'tensor'))
The draws below stay inside these ranges and needn't reach their ends.
Inputs may be any that keep to these rules, and one draw needn't show every extreme that they name: `tile_count`: some conversation has 2 tiles. `tile_owner`: entries with t at or past the conversation's count are -1. The tiles of one conversation have different owners, no two tiles share a slot, and some conv index holds 2 tiles. `visible`: never falls along a conversation's text; it is 0 at the first token and 2 at the last.
All inputs are finite; a program needn't handle non-finite values.
Results may differ from the reference program's by a relative error of at most 0.02.
Values may be sent and summed in bfloat16 or wider, within the bound.
A program may use at most 128 MiB of HBM per device.

```python
import math
import jax
import jax.numpy as jnp
from jax import lax

HD = 128
QHEADS = 32
KVHEADS = 8
MAXT = 2
TILE = 1601
TOK_SEQ = 128
GROUP = 4
TILE_PAD = 1664
LENGTH = 512
N_CONV = 4
N_SEQ = 4


def tile_plan(key):
    plan_key = jax.random.fold_in(key, 11)
    key_rows, key_cols, key_names, key_full, key_counts = jax.random.split(plan_key, 5)
    row_shift = jax.random.permutation(key_rows, N_CONV)
    col_shift = jax.random.permutation(key_cols, N_CONV)[:MAXT]
    relabel = jax.random.permutation(key_names, N_CONV)
    owners = relabel[(row_shift[:, None] + col_shift[None, :]) % N_CONV]
    full_owner = jax.random.randint(key_full, (), 0, N_CONV)
    tile_ids = jnp.arange(MAXT, dtype=jnp.int32)
    needed = jnp.max(jnp.where(owners == full_owner, tile_ids[None, :] + 1, 0), axis=1)
    counts = jnp.maximum(jax.random.randint(key_counts, (N_CONV,), 1, MAXT + 1), needed)
    owner_table = jnp.where(tile_ids[None, :] < counts[:, None], owners, -1)
    return (counts.astype(jnp.int32), owner_table.astype(jnp.int32))


def draw_tile_count(key, part):
    return tile_plan(key)[0]


def draw_tile_owner(key, part):
    return tile_plan(key)[1]


def draw_visible(key, part):
    thresholds = jax.random.randint(jax.random.fold_in(key, 23), (N_CONV, MAXT), 1, LENGTH)
    positions = jnp.arange(LENGTH, dtype=jnp.int32)
    return jnp.sum(thresholds[:, :, None] <= positions[None, None, :], axis=1).astype(jnp.int32)


def level_of(rng, dims, cuts, smallest, largest):
    loudness = 1.0
    for position, blocks in cuts:
        steps = jax.random.uniform(jax.random.fold_in(jax.random.fold_in(rng, 6), position), (blocks,), jnp.float32, smallest / len(cuts), largest / len(cuts))
        loudness = loudness * jnp.repeat(jnp.exp(steps), dims[position] // blocks).reshape((-1,) + (1,) * (len(dims) - 1 - position))
    return loudness


def centred(key, shape, deviation, limit, pieces=(), kind=jnp.bfloat16):
    values = jax.random.normal(key, shape, jnp.float32) * deviation
    if len(pieces) > 0:
        values = level_of(key, shape, pieces, -0.22, 0.18) * values
    return jnp.clip(values, min=-limit, max=limit).astype(kind)


def setup_inputs(seed: int = 0) -> dict:
    seeds = jax.random.split(jax.random.key(seed), 11)
    queries = centred(seeds[0], (N_CONV, LENGTH, QHEADS * HD), 1.0, 6.0, ((0, 4), (1, 4), (2, 2)))
    keys = centred(seeds[1], (N_CONV * MAXT, TILE_PAD, KVHEADS * HD), 1.0, 6.0, ((0, 4), (1, 8)))
    values = centred(seeds[2], (N_CONV * MAXT, TILE_PAD, KVHEADS * HD), 3.0, 18.0, ((0, 4), (1, 8)))
    q_gain = jnp.clip(jnp.exp(jax.random.uniform(seeds[3], (HD,), jnp.float32, math.log(0.9), math.log(2.2))), 0.9, 2.2)
    k_gain = jnp.clip(jnp.exp(jax.random.uniform(seeds[4], (HD,), jnp.float32, math.log(0.9), math.log(2.2))), 0.9, 2.2)
    gate = jnp.clip(jax.random.uniform(seeds[5], (1,), jnp.float32, 0.4, 1.6), 0.4, 1.6)
    tile_count = draw_tile_count(jax.random.fold_in(seeds[10], 71), 0)
    tile_owner = draw_tile_owner(jax.random.fold_in(seeds[10], 71), 0)
    visible = draw_visible(jax.random.fold_in(seeds[10], 71), 0)
    d_out = centred(seeds[9], (N_CONV, LENGTH, QHEADS * HD), 2.0, 12.0, ((0, 4), (1, 4), (2, 2)))
    return dict(queries=queries, keys=keys, values=values, q_gain=q_gain, k_gain=k_gain, gate=gate, tile_count=tile_count, tile_owner=tile_owner, visible=visible, d_out=d_out)


EPSILON = 1e-05

def head_norm(inputs, norm_gain):
    mean_square = lax.optimization_barrier(jnp.mean(inputs * inputs, axis=-1, keepdims=True))
    return inputs * lax.rsqrt(mean_square + EPSILON) * norm_gain

def rounded(inputs):
    return lax.optimization_barrier(inputs.astype(jnp.bfloat16)).astype(jnp.float32)

def reference(queries, keys, values, q_gain, k_gain, gate, tile_count, tile_owner, visible, d_out):
    score_scale = 1.0 / math.sqrt(HD)
    gate_value = jnp.tanh(gate[0])
    slots_all = N_CONV * MAXT
    key_raw = keys.astype(jnp.float32).reshape(slots_all, TILE_PAD, KVHEADS, HD)
    key_normed, key_back = jax.vjp(lambda inputs: head_norm(inputs, k_gain), key_raw)
    key_halfprec = key_normed.astype(jnp.bfloat16)
    value_all = values.reshape(slots_all, TILE_PAD, KVHEADS, HD)
    tile_ids = jnp.arange(MAXT, dtype=jnp.int32)
    row_ids = jnp.arange(TILE_PAD, dtype=jnp.int32)
    valid = tile_owner >= 0
    slot_index = jnp.where(valid, tile_owner * MAXT + tile_ids[None, :], 0).astype(jnp.int32)
    key_tile_ids = jnp.repeat(tile_ids, TILE_PAD)
    key_row_ids = jnp.tile(row_ids, MAXT)

    def one_conversation(conversation):
        chosen = slot_index[conversation]
        present = valid[conversation]
        tile_keys = jnp.where(present[:, None, None, None], key_halfprec[chosen], jnp.zeros((), jnp.bfloat16))
        tile_values = jnp.where(present[:, None, None, None], value_all[chosen], jnp.zeros((), jnp.bfloat16))
        flat_keys = tile_keys.reshape(MAXT * TILE_PAD, KVHEADS, HD).astype(jnp.float32)
        flat_values = tile_values.reshape(MAXT * TILE_PAD, KVHEADS, HD).astype(jnp.float32)
        seen_tiles = jnp.minimum(visible[conversation], tile_count[conversation])
        query_blocks = queries[conversation].astype(jnp.float32).reshape(N_SEQ, TOK_SEQ, QHEADS, HD)
        grad_blocks = d_out[conversation].astype(jnp.float32).reshape(N_SEQ, TOK_SEQ, KVHEADS, GROUP, HD)
        seen_blocks = seen_tiles.reshape(N_SEQ, TOK_SEQ)

        def one_block(carry, inputs):
            key_sum, value_sum = carry
            query_raw, cotangent, seen_here = inputs
            query_normed, query_back = jax.vjp(lambda vector: head_norm(vector, q_gain), query_raw)
            query_bf = rounded(query_normed).reshape(TOK_SEQ, KVHEADS, GROUP, HD)
            visible_keys = (key_tile_ids[None, :] < seen_here[:, None]) & (key_row_ids[None, :] < TILE)
            scores = jnp.einsum('pkgd,rkd->kgpr', query_bf, flat_keys) * score_scale
            weights = jnp.where(visible_keys[None, None], jnp.exp(scores), 0.0)
            weight_sum = lax.optimization_barrier(jnp.sum(weights, axis=-1))
            weighted = jnp.einsum('kgpr,rkd->pkgd', rounded(weights), flat_values)
            safe_sum = jnp.where(weight_sum > 0, weight_sum, 1.0)
            context = weighted / jnp.transpose(safe_sum, (2, 0, 1))[..., None]
            attended = (gate_value * context).astype(jnp.bfloat16).reshape(TOK_SEQ, QHEADS * HD)
            grad_ctx = rounded(gate_value * cotangent)
            row_delta = jnp.transpose(lax.optimization_barrier(jnp.sum(grad_ctx * context, axis=-1)), (1, 2, 0))
            probability = weights / safe_sum[..., None]
            grad_prob = jnp.einsum('pkgd,rkd->kgpr', grad_ctx, flat_values)
            grad_score = rounded(probability * (grad_prob - row_delta[..., None]))
            grad_query = jnp.einsum('kgpr,rkd->pkgd', grad_score, flat_keys) * score_scale
            query_grad = query_back(grad_query.reshape(TOK_SEQ, QHEADS, HD))[0]
            query_grad = query_grad.astype(jnp.bfloat16).reshape(TOK_SEQ, QHEADS * HD)
            key_part = jnp.einsum('kgpr,pkgd->rkd', grad_score, query_bf) * score_scale
            value_part = jnp.einsum('kgpr,pkgd->rkd', rounded(probability), grad_ctx)
            key_sum = key_sum + rounded(key_part)
            value_sum = value_sum + rounded(value_part)
            return ((key_sum, value_sum), (attended, query_grad))
        zero_grads = jnp.zeros((MAXT * TILE_PAD, KVHEADS, HD), jnp.float32)
        (key_sum, value_sum), (attended, query_grad) = lax.scan(one_block, (zero_grads, zero_grads), (query_blocks, grad_blocks, seen_blocks))
        key_grad = key_sum.astype(jnp.bfloat16).reshape(MAXT, TILE_PAD, KVHEADS, HD)
        value_grad = value_sum.astype(jnp.bfloat16).reshape(MAXT, TILE_PAD, KVHEADS, HD)
        return (attended.reshape(LENGTH, QHEADS * HD), query_grad.reshape(LENGTH, QHEADS * HD), key_grad, value_grad)
    attended, d_queries, key_grad, value_grad = lax.map(one_conversation, jnp.arange(N_CONV, dtype=jnp.int32))
    target = jnp.where(valid, tile_owner * MAXT + tile_ids[None, :], slots_all).astype(jnp.int32).reshape(-1)
    positioned_keys = jnp.zeros((slots_all, TILE_PAD, KVHEADS, HD), jnp.float32)
    positioned_keys = positioned_keys.at[target].add(key_grad.reshape(slots_all, TILE_PAD, KVHEADS, HD).astype(jnp.float32), mode='drop')
    placed_values = jnp.zeros((slots_all, TILE_PAD, KVHEADS, HD), jnp.float32)
    placed_values = placed_values.at[target].add(value_grad.reshape(slots_all, TILE_PAD, KVHEADS, HD).astype(jnp.float32), mode='drop')
    d_keys = key_back(positioned_keys)[0].astype(jnp.bfloat16).reshape(slots_all, TILE_PAD, KVHEADS * HD)
    d_values = placed_values.astype(jnp.bfloat16).reshape(slots_all, TILE_PAD, KVHEADS * HD)
    return (attended, d_queries, d_keys, d_values)
```

```python
from functools import partial
import math

import jax
import jax.numpy as jnp
from jax import lax
from jax.experimental import pallas as pl
from jax.experimental.pallas import tpu as pltpu
from jax.sharding import PartitionSpec as P

TILE = 1601


EPSILON = 1e-05


def head_norm(inputs, norm_gain):
    mean_square = jnp.mean(inputs * inputs, axis=-1, keepdims=True)
    return inputs * lax.rsqrt(mean_square + EPSILON) * norm_gain


def key_mask(seen_tiles, tile_index, row_start, row_count):
    row_ids = row_start + jnp.arange(row_count, dtype=jnp.int32)
    return (seen_tiles > tile_index)[:, None] & (row_ids < TILE)[None, :]


def tile_weights(query_bf, key_tile, visible_keys, score_scale):
    scores = (
        jnp.einsum("pkgd,rkd->kgpr", query_bf, key_tile, preferred_element_type=jnp.float32)
        * score_scale
    )
    return jnp.where(visible_keys[None, None], jnp.exp(scores), 0.0)


def tile_forward(query_bf, key_tile, value_tile, visible_keys, score_scale):
    weights = tile_weights(query_bf, key_tile, visible_keys, score_scale)
    weighted = jnp.einsum(
        "kgpr,rkd->pkgd",
        weights.astype(jnp.bfloat16),
        value_tile,
        preferred_element_type=jnp.float32,
    )
    return (jnp.sum(weights, axis=-1), weighted)


def tile_gradients(
    query_bf,
    grad_bf,
    key_tile,
    value_tile,
    visible_keys,
    safe_sum,
    row_delta,
    score_scale,
    block_count,
):
    weights = tile_weights(query_bf, key_tile, visible_keys, score_scale)
    probability = weights / safe_sum[..., None]
    grad_prob = jnp.einsum(
        "pkgd,rkd->kgpr", grad_bf, value_tile, preferred_element_type=jnp.float32
    )
    grad_score = (probability * (grad_prob - row_delta[..., None])).astype(jnp.bfloat16)
    prob_bf = probability.astype(jnp.bfloat16)
    grad_query = (
        jnp.einsum("kgpr,rkd->pkgd", grad_score, key_tile, preferred_element_type=jnp.float32)
        * score_scale
    )
    kv_local, group_size, token_count, row_count = grad_score.shape
    head_size = query_bf.shape[-1]
    block_tokens = token_count // block_count
    score_blocks = grad_score.reshape(kv_local, group_size, block_count, block_tokens, row_count)
    prob_blocks = prob_bf.reshape(kv_local, group_size, block_count, block_tokens, row_count)
    query_blocks = query_bf.reshape(block_count, block_tokens, kv_local, group_size, head_size)
    grad_blocks = grad_bf.reshape(block_count, block_tokens, kv_local, group_size, head_size)
    key_part = (
        jnp.einsum(
            "kgbpr,bpkgd->brkd", score_blocks, query_blocks, preferred_element_type=jnp.float32
        )
        * score_scale
    )
    value_part = jnp.einsum(
        "kgbpr,bpkgd->brkd", prob_blocks, grad_blocks, preferred_element_type=jnp.float32
    )
    key_part = jnp.sum(
        lax.optimization_barrier(key_part.astype(jnp.bfloat16)).astype(jnp.float32), axis=0
    )
    value_part = jnp.sum(
        lax.optimization_barrier(value_part.astype(jnp.bfloat16)).astype(jnp.float32), axis=0
    )
    return (
        grad_query,
        key_part.reshape(row_count, kv_local * head_size),
        value_part.reshape(row_count, kv_local * head_size),
    )


def attend_forward(query_bf, tile_keys, tile_values, seen_tiles, row_start, score_scale):
    row_count, slot_count, features = tile_keys.shape
    token_count, kv_local, group_size, head_size = query_bf.shape
    weight_sum = jnp.zeros((kv_local, group_size, token_count), jnp.float32)
    weighted = jnp.zeros(query_bf.shape, jnp.float32)
    for tile_index in range(slot_count):
        key_tile = tile_keys[:, tile_index].reshape(row_count, kv_local, head_size)
        value_tile = tile_values[:, tile_index].reshape(row_count, kv_local, head_size)
        visible_keys = key_mask(seen_tiles, tile_index, row_start, row_count)
        work = partial(tile_forward, query_bf, key_tile, value_tile, visible_keys, score_scale)
        part_sum, part_weighted = work()
        weight_sum = weight_sum + part_sum
        weighted = weighted + part_weighted
    return (weight_sum, weighted)


def attend_backward(
    query_bf,
    grad_bf,
    tile_keys,
    tile_values,
    seen_tiles,
    row_start,
    safe_sum,
    row_delta,
    score_scale,
    block_tokens,
):
    row_count, slot_count, features = tile_keys.shape
    token_count, kv_local, group_size, head_size = query_bf.shape
    block_count = token_count // block_tokens
    grad_query = jnp.zeros(query_bf.shape, jnp.float32)
    key_parts = []
    value_parts = []
    for tile_index in range(slot_count):
        key_tile = tile_keys[:, tile_index].reshape(row_count, kv_local, head_size)
        value_tile = tile_values[:, tile_index].reshape(row_count, kv_local, head_size)
        visible_keys = key_mask(seen_tiles, tile_index, row_start, row_count)
        work = partial(
            tile_gradients,
            query_bf,
            grad_bf,
            key_tile,
            value_tile,
            visible_keys,
            safe_sum,
            row_delta,
            score_scale,
            block_count,
        )
        part_query, key_part, value_part = work()
        grad_query = grad_query + part_query
        key_parts.append(key_part)
        value_parts.append(value_part)
    return (grad_query, jnp.stack(key_parts, axis=1), jnp.stack(value_parts, axis=1))


def row_shards(queries, keys, values, q_gain, k_gain, gate, tile_count, tile_owner, visible, d_out):
    conv_count = lax.axis_size("conv")
    tensor_count = lax.axis_size("tensor")
    conv_index = lax.axis_index("conv")
    sequence_index = lax.axis_index("seq")
    slot_count, row_local, features = keys.shape
    head_size = q_gain.shape[0]
    kv_heads = features // head_size
    kv_local = kv_heads // tensor_count
    token_count = queries.shape[1]
    query_heads = queries.shape[2] // head_size
    group_size = query_heads // kv_local
    score_scale = 1.0 / math.sqrt(head_size)
    gate_value = jnp.tanh(gate[0])
    conv_ids = jnp.arange(conv_count, dtype=jnp.int32)
    transfers = (tile_owner == conv_index).astype(jnp.bfloat16)
    own_owners = lax.dynamic_index_in_dim(tile_owner, conv_index, 0, keepdims=False)
    takes = (own_owners[:, None] == conv_ids[None, :]).astype(jnp.bfloat16)
    own_count = lax.dynamic_index_in_dim(tile_count, conv_index, 0, keepdims=False)
    seen_all = jnp.minimum(
        lax.dynamic_index_in_dim(visible, conv_index, 0, keepdims=False), own_count
    )
    key_raw = keys.astype(jnp.float32).reshape(slot_count, row_local, kv_heads, head_size)
    key_normed, key_back = jax.vjp(lambda inputs: head_norm(inputs, k_gain), key_raw)
    key_halfprec = key_normed.astype(jnp.bfloat16).reshape(slot_count, row_local, features)
    outgoing_keys = jnp.einsum(
        "wn,nki->wki", transfers, key_halfprec, preferred_element_type=jnp.float32
    ).astype(jnp.bfloat16)
    send_values = jnp.einsum(
        "wn,nki->wki", transfers, values, preferred_element_type=jnp.float32
    ).astype(jnp.bfloat16)
    got_keys, got_values = (
        lax.all_to_all(
            lax.all_to_all(outgoing_keys, "conv", split_axis=0, concat_axis=0, tiled=True),
            "tensor",
            split_axis=2,
            concat_axis=1,
            tiled=True,
        ),
        lax.all_to_all(
            lax.all_to_all(send_values, "conv", split_axis=0, concat_axis=0, tiled=True),
            "tensor",
            split_axis=2,
            concat_axis=1,
            tiled=True,
        ),
    )
    tile_keys = jnp.einsum(
        "to,orf->rtf", takes, got_keys, preferred_element_type=jnp.float32
    ).astype(jnp.bfloat16)
    tile_values = jnp.einsum(
        "to,orf->rtf", takes, got_values, preferred_element_type=jnp.float32
    ).astype(jnp.bfloat16)
    query_raw = queries[0].astype(jnp.float32).reshape(token_count, query_heads, head_size)
    query_normed, query_back = jax.vjp(lambda inputs: head_norm(inputs, q_gain), query_raw)
    query_bf = query_normed.astype(jnp.bfloat16).reshape(
        token_count, kv_local, group_size, head_size
    )
    grad_bf = (
        (gate_value * d_out[0].astype(jnp.float32))
        .astype(jnp.bfloat16)
        .reshape(token_count, kv_local, group_size, head_size)
    )
    own_start = sequence_index * token_count
    all_queries = lax.all_gather(query_bf, "seq", axis=0, tiled=True)
    all_grads = lax.all_gather(grad_bf, "seq", axis=0, tiled=True)
    share_rows = tile_keys.shape[0]
    row_start = sequence_index * share_rows
    part_sum, part_weighted = attend_forward(
        all_queries, tile_keys, tile_values, seen_all, row_start, score_scale
    )
    all_weighted, all_weight_sum = (
        lax.psum(part_weighted.astype(jnp.bfloat16), "seq").astype(jnp.float32),
        lax.psum(part_sum.astype(jnp.bfloat16), "seq").astype(jnp.float32),
    )
    safe_all = jnp.where(all_weight_sum > 0, all_weight_sum, 1.0)
    context_all = all_weighted / jnp.transpose(safe_all, (2, 0, 1))[..., None]
    context = lax.dynamic_slice_in_dim(context_all, own_start, token_count, 0)
    row_delta = jnp.transpose(
        jnp.sum(all_grads.astype(jnp.float32) * context_all, axis=-1), (1, 2, 0)
    )
    grad_part, key_sums, value_sums = attend_backward(
        all_queries,
        all_grads,
        tile_keys,
        tile_values,
        seen_all,
        row_start,
        safe_all,
        row_delta,
        score_scale,
        token_count,
    )
    grad_query = lax.psum_scatter(
        grad_part.astype(jnp.bfloat16), "seq", scatter_dimension=0, tiled=True
    ).astype(jnp.float32)
    attended = (
        (gate_value * context).astype(jnp.bfloat16).reshape(1, token_count, query_heads * head_size)
    )
    key_round = key_sums.astype(jnp.bfloat16)
    value_round = value_sums.astype(jnp.bfloat16)
    back_keys = jnp.einsum(
        "to,rtf->orf", takes, key_round, preferred_element_type=jnp.float32
    ).astype(jnp.bfloat16)
    back_values = jnp.einsum(
        "to,rtf->orf", takes, value_round, preferred_element_type=jnp.float32
    ).astype(jnp.bfloat16)
    returned_keys, returned_values = (
        lax.all_to_all(
            lax.all_to_all(back_keys, "conv", split_axis=0, concat_axis=0, tiled=True),
            "tensor",
            split_axis=1,
            concat_axis=2,
            tiled=True,
        ),
        lax.all_to_all(
            lax.all_to_all(back_values, "conv", split_axis=0, concat_axis=0, tiled=True),
            "tensor",
            split_axis=1,
            concat_axis=2,
            tiled=True,
        ),
    )
    positioned_keys = jnp.einsum(
        "ew,eig->wig", transfers, returned_keys, preferred_element_type=jnp.float32
    )
    d_values = jnp.einsum(
        "ew,eig->wig", transfers, returned_values, preferred_element_type=jnp.float32
    ).astype(jnp.bfloat16)
    d_keys = key_back(positioned_keys.reshape(slot_count, row_local, kv_heads, head_size))[0]
    d_keys = d_keys.astype(jnp.bfloat16).reshape(slot_count, row_local, features)
    d_queries = query_back(grad_query.reshape(token_count, query_heads, head_size))[0]
    d_queries = d_queries.astype(jnp.bfloat16).reshape(1, token_count, query_heads * head_size)
    return (attended, d_queries, d_keys, d_values)


LOG2E = math.log2(math.e)


def row_chunks(rows):
    starts = list(range(0, max(rows - 511, 1), 512))
    return [(a, b - a) for a, b in zip(starts, starts[1:] + [rows])]


def inverse_rms(inputs):
    return lax.rsqrt(jnp.mean(inputs * inputs, axis=-1, keepdims=True) + EPSILON)


def norm_back(inputs, inv, gained):
    return inv * gained - inputs * (inv * inv * inv) * jnp.mean(
        inputs * gained, axis=-1, keepdims=True
    )


def dot(lhs, rhs):
    return jnp.dot(lhs, rhs, preferred_element_type=jnp.float32)


def head_kernel(
    owners, counts, gate, visible, q_gain_ref, k_gain_ref, q_hbm, do_hbm, k_hbm, v_hbm,
    att_hbm, dq_hbm, ret_hbm,
    kv, qa, da, seen, kr, kn, kt, vn, vt, wts, qs, qst, dos, dost, acc, total, dqt, dk, dv,
    att_st, dq_st, gr, ret,
    kv_send, kv_recv, own_sem, conv_send, conv_recv, relay_send, relay_recv,
    q_send, q_recv, own_q_sem, out_send, out_recv, own_out_sem,
    gr_send, gr_recv, back_send, back_recv, backrelay_send, backrelay_recv, ret_sem,
    *, conv_count, seq_count, tensor_count,
):
    c = lax.axis_index("conv")
    z = lax.axis_index("seq")
    x = lax.axis_index("tensor")
    tiles, row_local, features = k_hbm.shape
    size = q_gain_ref.shape[1]
    rows = kn.shape[1]
    count = q_hbm.shape[0]
    width = qa.shape[2]
    group = width // size
    heads_side = features // size // tensor_count
    scale = 1.0 / math.sqrt(size)

    def at(conv, seq, tensor):
        return {"conv": conv, "seq": seq, "tensor": tensor}

    def remote(src, dst, send, recv, device):
        return pltpu.make_async_remote_copy(
            src_ref=src, dst_ref=dst, send_sem=send, recv_sem=recv,
            device_id=device, device_id_type=pl.DeviceIdType.MESH,
        )

    partner = c + 1 - 2 * lax.rem(c, 2)
    siblings = [lax.rem(c + 2 * m, conv_count) for m in range(1, conv_count // 2)]
    far_first = sorted(range(1, seq_count), key=lambda k: -min(k, seq_count - k))
    offsets = [(0, e) for e in range(tensor_count)]
    offsets += [(k, e) for k in far_first for e in range(tensor_count)]

    def target(offset):
        k, e = offset
        return lax.rem(z + k, seq_count), lax.rem(x + e, tensor_count)

    def source(offset):
        k, e = offset
        return lax.rem(z + seq_count - k, seq_count), lax.rem(x + tensor_count - e, tensor_count)

    def block_rows(seq, tensor):
        start = (seq * tensor_count + tensor) * row_local
        return pl.ds(pl.multiple_of(start, 16), row_local)

    def head_lanes(seq, tensor):
        return pl.ds(pl.multiple_of((tensor * heads_side + seq) * size, size), size)

    def group_lanes(seq):
        return pl.ds(pl.multiple_of(seq * width, width), width)

    barrier = pltpu.get_barrier_semaphore()
    peers = [at(c, *target(offset)) for offset in offsets[1:]]
    peers += [at(other, z, x) for other in [partner] + siblings]
    for peer in peers:
        pl.semaphore_signal(barrier, inc=1, device_id=peer, device_id_type=pl.DeviceIdType.MESH)
    pl.semaphore_wait(barrier, len(peers))

    own_rows = block_rows(z, x)
    stores = (k_hbm, v_hbm)
    for j, offset in enumerate(offsets):
        to = target(offset)
        for part, store in enumerate(stores):
            src = store.at[:, :, head_lanes(*to)]
            dst = kv.at[c, part, :, own_rows, :]
            if j == 0:
                pltpu.make_async_copy(src, dst, own_sem.at[part]).start()
            else:
                remote(src, dst, kv_send.at[part, j], kv_recv.at[part, j], at(c, *to)).start()
    for part, (store, into) in enumerate(((q_hbm, qa), (do_hbm, da))):
        pltpu.make_async_copy(store.at[:, group_lanes(z)], into.at[z], own_q_sem.at[part]).start()

    def q_copy(part, k):
        store, into = ((q_hbm, qa), (do_hbm, da))[part]
        to = lax.rem(z + k, seq_count)
        return remote(
            store.at[:, group_lanes(to)], into.at[z],
            q_send.at[part, k], q_recv.at[part, seq_count - k], at(c, to, x),
        )

    for k in reversed(range(1, seq_count)):
        for part in range(2):
            q_copy(part, k).start()

    seen_all = jnp.minimum(visible[pl.ds(c, 1), :], counts[c])
    for b in range(seq_count):
        piece = seen_all[:, b * count:(b + 1) * count]
        seen[b] = jnp.concatenate([piece] * group, axis=1)
    dk[...] = jnp.zeros_like(dk)
    dv[...] = jnp.zeros_like(dv)
    q_gain = q_gain_ref[...]
    k_gain = k_gain_ref[...]
    gate_value = jnp.tanh(gate[...])

    def kv_view(j):
        place = block_rows(*source(offsets[j]))
        return lambda conv: kv.at[conv, :, :, place, :]

    def spread_start(view, j, send, recv):
        for n, to in enumerate([partner] + siblings):
            remote(view(c), view(c), send.at[n, j], recv.at[n, j], at(to, z, x)).start()

    def relay_start(view, j, send, recv, r_send, r_recv):
        for m, other in enumerate(siblings):
            came = conv_count // 2 - (m + 1)
            remote(view(c), view(other), send.at[m + 1, j], recv.at[came, j], at(c, z, x)).wait_recv()
            remote(view(other), view(other), r_send.at[m, j], r_recv.at[m, j], at(partner, z, x)).start()

    def spread_finish(view, j, send, recv, r_send, r_recv):
        remote(view(c), view(partner), send.at[0, j], recv.at[0, j], at(partner, z, x)).wait_recv()
        for n in range(len(siblings) + 1):
            remote(view(c), view(c), send.at[n, j], recv.at[n, j], at(partner, z, x)).wait_send()
        for m in range(len(siblings)):
            far = lax.rem(partner + 2 * (m + 1), conv_count)
            remote(view(far), view(far), r_send.at[m, j], r_recv.at[m, j], at(partner, z, x)).wait()

    for j, offset in enumerate(offsets):
        place = block_rows(*source(offset))
        for part, store in enumerate(stores):
            dst = kv.at[c, part, :, place, :]
            src = store.at[:, :, head_lanes(z, x)]
            if j == 0:
                pltpu.make_async_copy(src, dst, own_sem.at[part]).wait()
            else:
                remote(
                    src, dst, kv_send.at[part, j], kv_recv.at[part, j], at(c, z, x)
                ).wait_recv()
        spread_start(kv_view(j), j, conv_send, conv_recv)
        if j > 0:
            relay_start(kv_view(j - 1), j - 1, conv_send, conv_recv, relay_send, relay_recv)
    last = len(offsets) - 1
    relay_start(kv_view(last), last, conv_send, conv_recv, relay_send, relay_recv)
    for j in range(len(offsets)):
        spread_finish(kv_view(j), j, conv_send, conv_recv, relay_send, relay_recv)

    for tile in range(tiles):
        owner = owners[c, tile]

        @pl.loop(0, rows // 128)
        def _(step, tile=tile, owner=owner):
            here = pl.ds(pl.multiple_of(step * 128, 128), 128)

            def chosen(part):
                value = kv[0, part, tile, here, :]
                for conv in range(1, conv_count):
                    value = jnp.where(owner == conv, kv[conv, part, tile, here, :], value)
                return value

            raw_bf = chosen(0)
            raw = raw_bf.astype(jnp.float32)
            normed = raw * inverse_rms(raw) * k_gain
            kr[tile, here, :] = raw_bf
            kn[tile, here, :] = normed.astype(jnp.bfloat16)
            kt[tile, :, here] = normed.T.astype(jnp.bfloat16)
            value = chosen(1)
            vn[tile, here, :] = value
            vt[tile, :, here] = value.astype(jnp.float32).T.astype(jnp.bfloat16)

    chunks = row_chunks(rows)

    def out_copy(part, i):
        stage, out = ((att_st, att_hbm), (dq_st, dq_hbm))[part]
        to = lax.rem(z + i, seq_count)
        return remote(
            stage.at[to], out.at[:, group_lanes(z)],
            out_send.at[part, i], out_recv.at[part, seq_count - i], at(c, to, x),
        )

    @pl.loop(0, seq_count)
    def _(i):
        block = lax.rem(z + i, seq_count)

        @pl.when(i == 0)
        def _():
            for part, (store, into) in enumerate(((q_hbm, qa), (do_hbm, da))):
                pltpu.make_async_copy(
                    store.at[:, group_lanes(z)], into.at[z], own_q_sem.at[part]
                ).wait()

        @pl.when(i > 0)
        def _():
            for part, (store, into) in enumerate(((q_hbm, qa), (do_hbm, da))):
                remote(
                    store.at[:, group_lanes(z)], into.at[block],
                    q_send.at[part, i], q_recv.at[part, i], at(c, block, x),
                ).wait_recv()

        for g in range(group):
            raw = qa[block, :, pl.ds(g * size, size)].astype(jnp.float32)
            normed = raw * inverse_rms(raw) * (q_gain * (scale * LOG2E))
            qs[pl.ds(g * count, count), :] = normed.astype(jnp.bfloat16)
            qst[:, pl.ds(g * count, count)] = normed.T.astype(jnp.bfloat16)
        seen_row = seen[block]
        acc[...] = jnp.zeros_like(acc)
        total[...] = jnp.zeros_like(total)
        dqt[...] = jnp.zeros_like(dqt)

        @pl.loop(0, tiles)
        def _(tile):
            mask = (seen_row > tile).astype(jnp.float32)
            part = jnp.zeros(acc.shape, jnp.float32)
            part_sum = jnp.zeros(total.shape, jnp.float32)
            for start, length in chunks:
                here = pl.ds(start, length)
                w = jnp.exp2(dot(kn[tile, here, :], qst[...]))
                if start + length > TILE:
                    ids = start + lax.broadcasted_iota(jnp.int32, w.shape, 0)
                    w = jnp.where(ids < TILE, w, 0.0)
                part_sum = part_sum + jnp.sum(w, axis=0, keepdims=True)
                w_bf = w.astype(jnp.bfloat16)
                wts[tile, here, :] = w_bf
                part = part + dot(vt[tile, :, here], w_bf)
            acc[...] += part * mask
            total[...] += part_sum * mask

        @pl.when(i > 1)
        def _():
            for part in range(2):
                out_copy(part, i - 1).start()

        safe = jnp.where(total[...] > 0, total[...], 1.0)
        inv = 1.0 / safe
        ctx = acc[...] * inv
        for g in range(group):
            lanes = pl.ds(g * count, count)
            grad = da[block, :, pl.ds(g * size, size)].astype(jnp.float32) * gate_value
            dost[:, lanes] = grad.T
            att_st[block, :, pl.ds(g * size, size)] = (
                (gate_value * ctx[:, g * count:(g + 1) * count]).T.astype(jnp.bfloat16)
            )
        scaled = (dost[...] * inv).astype(jnp.bfloat16)
        scaled32 = scaled.astype(jnp.float32)
        delta = jnp.sum(scaled32 * ctx, axis=0, keepdims=True)

        @pl.loop(0, tiles)
        def _(tile):
            mask = (seen_row > tile).astype(jnp.float32)
            cut32 = scaled32 * mask
            cut = cut32.astype(jnp.bfloat16)
            for g in range(group):
                dos[pl.ds(g * count, count), :] = (
                    cut32[:, g * count:(g + 1) * count].T.astype(jnp.bfloat16)
                )
            low = delta * mask
            part = jnp.zeros(dqt.shape, jnp.float32)
            for start, length in chunks:
                here = pl.ds(start, length)
                w_bf = wts[tile, here, :]
                dp = dot(vn[tile, here, :], cut)
                ds = (w_bf.astype(jnp.float32) * (dp - low)).astype(jnp.bfloat16)
                dv[tile, here, :] += dot(w_bf, dos[...])
                dk[tile, here, :] += dot(ds, qs[...])
                part = part + dot(kt[tile, :, here], ds)
            dqt[...] += part

        for g in range(group):
            raw = qa[block, :, pl.ds(g * size, size)].astype(jnp.float32)
            grad = dqt[:, pl.ds(g * count, count)].T * (q_gain * scale)
            dq_st[block, :, pl.ds(g * size, size)] = norm_back(
                raw, inverse_rms(raw), grad
            ).astype(jnp.bfloat16)

    def gr_copy(j):
        to = target(offsets[j])
        return remote(
            gr.at[:, :, block_rows(*to), :], ret.at[c, :, :, :, head_lanes(z, x)],
            gr_send.at[j], gr_recv.at[j], at(c, *to),
        )

    order = list(range(2, len(offsets))) + [1, 0]
    for n, j in enumerate(order):
        place = block_rows(*target(offsets[j]))

        @pl.loop(0, tiles)
        def _(tile, place=place):
            raw = kr[tile, place, :].astype(jnp.float32)
            grad = dk[tile, place, :] * (1.0 / LOG2E) * k_gain
            gr[0, tile, place, :] = norm_back(raw, inverse_rms(raw), grad).astype(jnp.bfloat16)
            gr[1, tile, place, :] = dv[tile, place, :].astype(jnp.bfloat16)

        if n > 0:
            gr_copy(order[n - 1]).start()
    for part in range(2):
        out_copy(part, seq_count - 1).start()
    stages = ((att_st, att_hbm), (dq_st, dq_hbm))
    for part, (stage, out) in enumerate(stages):
        pltpu.make_async_copy(stage.at[z], out.at[:, group_lanes(z)], own_out_sem.at[part]).start()
    ret[c, :, :, :, head_lanes(z, x)] = gr[:, :, own_rows, :]

    def ret_view(j):
        lanes = head_lanes(*source(offsets[j]))
        return lambda conv: ret.at[conv, :, :, :, lanes]

    def ret_out(j):
        lanes = head_lanes(*source(offsets[j]))
        return pltpu.make_async_copy(
            ret.at[:, :, :, :, lanes], ret_hbm.at[:, :, :, :, lanes], ret_sem.at[j]
        )

    sems = (back_send, back_recv, backrelay_send, backrelay_recv)
    arrival = [1] + list(range(2, len(offsets)))
    arrival = list(range(2, 3)) + [0, 1] + list(range(3, len(offsets)))
    for n, j in enumerate(arrival):
        if j > 0:
            remote(
                gr.at[:, :, own_rows, :], ret_view(j)(c), gr_send.at[j], gr_recv.at[j], at(c, z, x)
            ).wait_recv()
        spread_start(ret_view(j), j, back_send, back_recv)
        if n > 0:
            relay_start(ret_view(arrival[n - 1]), arrival[n - 1], *sems)
        if n > 1:
            spread_finish(ret_view(arrival[n - 2]), arrival[n - 2], *sems)
            ret_out(arrival[n - 2]).start()
    relay_start(ret_view(arrival[-1]), arrival[-1], *sems)
    for j in arrival[-2:]:
        spread_finish(ret_view(j), j, *sems)
        ret_out(j).start()

    for part, (stage, out) in enumerate(stages):
        for i in range(1, seq_count):
            remote(
                stage.at[z], out.at[:, group_lanes(lax.rem(z + seq_count - i, seq_count))],
                out_send.at[part, i], out_recv.at[part, i], at(c, z, x),
            ).wait()
        pltpu.make_async_copy(stage.at[z], out.at[:, group_lanes(z)], own_out_sem.at[part]).wait()
    for j in range(1, len(offsets)):
        gr_copy(j).wait_send()
        for part, store in enumerate(stores):
            to = target(offsets[j])
            remote(
                store.at[:, :, head_lanes(*to)], kv.at[c, part, :, own_rows, :],
                kv_send.at[part, j], kv_recv.at[part, j], at(c, *to),
            ).wait_send()
    for k in range(1, seq_count):
        for part in range(2):
            q_copy(part, k).wait_send()
    for j in range(len(offsets)):
        ret_out(j).wait()


def head_shards(queries, keys, values, q_gain, k_gain, gate, tile_count, tile_owner, visible, d_out):
    conv_count = lax.axis_size("conv")
    tensor_count = lax.axis_size("tensor")
    seq_count = lax.axis_size("seq")
    conv_index = lax.axis_index("conv")
    slot_count, row_local, features = keys.shape
    size = q_gain.shape[0]
    block_tokens, width_all = queries.shape[1:]
    width = width_all // seq_count
    lanes = width // size * block_tokens
    rows = row_local * seq_count * tensor_count
    bf, f32 = jnp.bfloat16, jnp.float32
    parts = seq_count * tensor_count
    far = conv_count // 2 - 1
    dma = pltpu.SemaphoreType.DMA

    vmem = pl.BlockSpec(memory_space=pltpu.VMEM)
    smem = pl.BlockSpec(memory_space=pltpu.SMEM)
    hbm = pl.BlockSpec(memory_space=pl.ANY)
    att, dq, ret = pl.pallas_call(
        partial(
            head_kernel, conv_count=conv_count, seq_count=seq_count, tensor_count=tensor_count
        ),
        out_shape=[jax.ShapeDtypeStruct((block_tokens, width_all), bf)] * 2
        + [jax.ShapeDtypeStruct((conv_count, 2, slot_count, row_local, features), bf)],
        in_specs=[smem] * 2 + [vmem] * 4 + [hbm] * 4,
        out_specs=[hbm] * 3,
        scratch_shapes=[
            pltpu.VMEM((conv_count, 2, slot_count, rows, size), bf),
            pltpu.VMEM((seq_count, block_tokens, width), bf),
            pltpu.VMEM((seq_count, block_tokens, width), bf),
            pltpu.VMEM((seq_count, 1, lanes), jnp.int32),
            pltpu.VMEM((slot_count, rows, size), bf),
            pltpu.VMEM((slot_count, rows, size), bf),
            pltpu.VMEM((slot_count, size, rows), bf),
            pltpu.VMEM((slot_count, rows, size), bf),
            pltpu.VMEM((slot_count, size, rows), bf),
            pltpu.VMEM((slot_count, rows, lanes), bf),
            pltpu.VMEM((lanes, size), bf),
            pltpu.VMEM((size, lanes), bf),
            pltpu.VMEM((lanes, size), bf),
            pltpu.VMEM((size, lanes), f32),
            pltpu.VMEM((size, lanes), f32),
            pltpu.VMEM((1, lanes), f32),
            pltpu.VMEM((size, lanes), f32),
            pltpu.VMEM((slot_count, rows, size), f32),
            pltpu.VMEM((slot_count, rows, size), f32),
            pltpu.VMEM((seq_count, block_tokens, width), bf),
            pltpu.VMEM((seq_count, block_tokens, width), bf),
            pltpu.VMEM((2, slot_count, rows, size), bf),
            pltpu.VMEM((conv_count, 2, slot_count, row_local, features), bf),
            dma((2, parts)), dma((2, parts)), dma((2,)),
            dma((far + 1, parts)), dma((far + 1, parts)), dma((far, parts)), dma((far, parts)),
            dma((2, seq_count)), dma((2, seq_count)), dma((2,)),
            dma((2, seq_count)), dma((2, seq_count)), dma((2,)),
            dma((parts,)), dma((parts,)),
            dma((far + 1, parts)), dma((far + 1, parts)), dma((far, parts)), dma((far, parts)),
            dma((parts,)),
        ],
        compiler_params=pltpu.CompilerParams(
            collective_id=0, has_side_effects=True, vmem_limit_bytes=60 << 20
        ),
    )(
        tile_owner, tile_count, gate.reshape(1, 1), visible, q_gain[None], k_gain[None],
        queries[0], d_out[0], keys, values,
    )

    goes = tile_owner == conv_index
    taker = jnp.argmax(goes, axis=0)
    used = jnp.any(goes, axis=0)
    zero = jnp.zeros((), bf)

    def placed(part):
        return jnp.stack(
            [
                jnp.where(
                    used[slot],
                    lax.dynamic_index_in_dim(ret[:, part, slot], taker[slot], 0, keepdims=False),
                    zero,
                )
                for slot in range(slot_count)
            ]
        )

    return (att[None], dq[None], placed(0), placed(1))


def shards(queries, keys, *rest):
    heads = keys.shape[2] // rest[1].shape[0]
    seq_count, tensor_count = lax.axis_size("seq"), lax.axis_size("tensor")
    conv_count = lax.axis_size("conv")
    split = seq_count * tensor_count
    fits = heads == split and conv_count % 2 == 0 and conv_count > 2
    fits = fits and keys.shape[1] * split % 128 == 0
    return (head_shards if fits else row_shards)(queries, keys, *rest)


def solution(mesh):
    in_specs = (
        P("conv", "seq", "tensor"),
        P("conv", ("seq", "tensor"), None),
        P("conv", ("seq", "tensor"), None),
        P(),
        P(),
        P(),
        P(),
        P(),
        P(),
        P("conv", "seq", "tensor"),
    )
    out_specs = (
        P("conv", "seq", "tensor"),
        P("conv", "seq", "tensor"),
        P("conv", ("seq", "tensor"), None),
        P("conv", ("seq", "tensor"), None),
    )
    return jax.shard_map(shards, mesh=mesh, in_specs=in_specs, out_specs=out_specs, check_vma=False)
```

```python
from functools import partial
import math

import jax
import jax.numpy as jnp
from jax import lax
from jax.experimental import pallas as pl
from jax.experimental.pallas import tpu as pltpu
from jax.sharding import PartitionSpec as P

TILE = 1601


EPSILON = 1e-05


def head_norm(inputs, norm_gain):
    mean_square = jnp.mean(inputs * inputs, axis=-1, keepdims=True)
    return inputs * lax.rsqrt(mean_square + EPSILON) * norm_gain


def key_mask(seen_tiles, tile_index, row_start, row_count):
    row_ids = row_start + jnp.arange(row_count, dtype=jnp.int32)
    return (seen_tiles > tile_index)[:, None] & (row_ids < TILE)[None, :]


def tile_weights(query_bf, key_tile, visible_keys, score_scale):
    scores = (
        jnp.einsum("pkgd,rkd->kgpr", query_bf, key_tile, preferred_element_type=jnp.float32)
        * score_scale
    )
    return jnp.where(visible_keys[None, None], jnp.exp(scores), 0.0)


def tile_forward(query_bf, key_tile, value_tile, visible_keys, score_scale):
    weights = tile_weights(query_bf, key_tile, visible_keys, score_scale)
    weighted = jnp.einsum(
        "kgpr,rkd->pkgd",
        weights.astype(jnp.bfloat16),
        value_tile,
        preferred_element_type=jnp.float32,
    )
    return (jnp.sum(weights, axis=-1), weighted)


def tile_gradients(
    query_bf,
    grad_bf,
    key_tile,
    value_tile,
    visible_keys,
    safe_sum,
    row_delta,
    score_scale,
    block_count,
):
    weights = tile_weights(query_bf, key_tile, visible_keys, score_scale)
    probability = weights / safe_sum[..., None]
    grad_prob = jnp.einsum(
        "pkgd,rkd->kgpr", grad_bf, value_tile, preferred_element_type=jnp.float32
    )
    grad_score = (probability * (grad_prob - row_delta[..., None])).astype(jnp.bfloat16)
    prob_bf = probability.astype(jnp.bfloat16)
    grad_query = (
        jnp.einsum("kgpr,rkd->pkgd", grad_score, key_tile, preferred_element_type=jnp.float32)
        * score_scale
    )
    kv_local, group_size, token_count, row_count = grad_score.shape
    head_size = query_bf.shape[-1]
    block_tokens = token_count // block_count
    score_blocks = grad_score.reshape(kv_local, group_size, block_count, block_tokens, row_count)
    prob_blocks = prob_bf.reshape(kv_local, group_size, block_count, block_tokens, row_count)
    query_blocks = query_bf.reshape(block_count, block_tokens, kv_local, group_size, head_size)
    grad_blocks = grad_bf.reshape(block_count, block_tokens, kv_local, group_size, head_size)
    key_part = (
        jnp.einsum(
            "kgbpr,bpkgd->brkd", score_blocks, query_blocks, preferred_element_type=jnp.float32
        )
        * score_scale
    )
    value_part = jnp.einsum(
        "kgbpr,bpkgd->brkd", prob_blocks, grad_blocks, preferred_element_type=jnp.float32
    )
    key_part = jnp.sum(
        lax.optimization_barrier(key_part.astype(jnp.bfloat16)).astype(jnp.float32), axis=0
    )
    value_part = jnp.sum(
        lax.optimization_barrier(value_part.astype(jnp.bfloat16)).astype(jnp.float32), axis=0
    )
    return (
        grad_query,
        key_part.reshape(row_count, kv_local * head_size),
        value_part.reshape(row_count, kv_local * head_size),
    )


def attend_forward(query_bf, tile_keys, tile_values, seen_tiles, row_start, score_scale):
    row_count, slot_count, features = tile_keys.shape
    token_count, kv_local, group_size, head_size = query_bf.shape
    weight_sum = jnp.zeros((kv_local, group_size, token_count), jnp.float32)
    weighted = jnp.zeros(query_bf.shape, jnp.float32)
    for tile_index in range(slot_count):
        key_tile = tile_keys[:, tile_index].reshape(row_count, kv_local, head_size)
        value_tile = tile_values[:, tile_index].reshape(row_count, kv_local, head_size)
        visible_keys = key_mask(seen_tiles, tile_index, row_start, row_count)
        work = partial(tile_forward, query_bf, key_tile, value_tile, visible_keys, score_scale)
        part_sum, part_weighted = work()
        weight_sum = weight_sum + part_sum
        weighted = weighted + part_weighted
    return (weight_sum, weighted)


def attend_backward(
    query_bf,
    grad_bf,
    tile_keys,
    tile_values,
    seen_tiles,
    row_start,
    safe_sum,
    row_delta,
    score_scale,
    block_tokens,
):
    row_count, slot_count, features = tile_keys.shape
    token_count, kv_local, group_size, head_size = query_bf.shape
    block_count = token_count // block_tokens
    grad_query = jnp.zeros(query_bf.shape, jnp.float32)
    key_parts = []
    value_parts = []
    for tile_index in range(slot_count):
        key_tile = tile_keys[:, tile_index].reshape(row_count, kv_local, head_size)
        value_tile = tile_values[:, tile_index].reshape(row_count, kv_local, head_size)
        visible_keys = key_mask(seen_tiles, tile_index, row_start, row_count)
        work = partial(
            tile_gradients,
            query_bf,
            grad_bf,
            key_tile,
            value_tile,
            visible_keys,
            safe_sum,
            row_delta,
            score_scale,
            block_count,
        )
        part_query, key_part, value_part = work()
        grad_query = grad_query + part_query
        key_parts.append(key_part)
        value_parts.append(value_part)
    return (grad_query, jnp.stack(key_parts, axis=1), jnp.stack(value_parts, axis=1))


def row_shards(queries, keys, values, q_gain, k_gain, gate, tile_count, tile_owner, visible, d_out):
    conv_count = lax.axis_size("conv")
    tensor_count = lax.axis_size("tensor")
    conv_index = lax.axis_index("conv")
    sequence_index = lax.axis_index("seq")
    slot_count, row_local, features = keys.shape
    head_size = q_gain.shape[0]
    kv_heads = features // head_size
    kv_local = kv_heads // tensor_count
    token_count = queries.shape[1]
    query_heads = queries.shape[2] // head_size
    group_size = query_heads // kv_local
    score_scale = 1.0 / math.sqrt(head_size)
    gate_value = jnp.tanh(gate[0])
    conv_ids = jnp.arange(conv_count, dtype=jnp.int32)
    transfers = (tile_owner == conv_index).astype(jnp.bfloat16)
    own_owners = lax.dynamic_index_in_dim(tile_owner, conv_index, 0, keepdims=False)
    takes = (own_owners[:, None] == conv_ids[None, :]).astype(jnp.bfloat16)
    own_count = lax.dynamic_index_in_dim(tile_count, conv_index, 0, keepdims=False)
    seen_all = jnp.minimum(
        lax.dynamic_index_in_dim(visible, conv_index, 0, keepdims=False), own_count
    )
    key_raw = keys.astype(jnp.float32).reshape(slot_count, row_local, kv_heads, head_size)
    key_normed, key_back = jax.vjp(lambda inputs: head_norm(inputs, k_gain), key_raw)
    key_halfprec = key_normed.astype(jnp.bfloat16).reshape(slot_count, row_local, features)
    outgoing_keys = jnp.einsum(
        "wn,nki->wki", transfers, key_halfprec, preferred_element_type=jnp.float32
    ).astype(jnp.bfloat16)
    send_values = jnp.einsum(
        "wn,nki->wki", transfers, values, preferred_element_type=jnp.float32
    ).astype(jnp.bfloat16)
    got_keys, got_values = (
        lax.all_to_all(
            lax.all_to_all(outgoing_keys, "conv", split_axis=0, concat_axis=0, tiled=True),
            "tensor",
            split_axis=2,
            concat_axis=1,
            tiled=True,
        ),
        lax.all_to_all(
            lax.all_to_all(send_values, "conv", split_axis=0, concat_axis=0, tiled=True),
            "tensor",
            split_axis=2,
            concat_axis=1,
            tiled=True,
        ),
    )
    tile_keys = jnp.einsum(
        "to,orf->rtf", takes, got_keys, preferred_element_type=jnp.float32
    ).astype(jnp.bfloat16)
    tile_values = jnp.einsum(
        "to,orf->rtf", takes, got_values, preferred_element_type=jnp.float32
    ).astype(jnp.bfloat16)
    query_raw = queries[0].astype(jnp.float32).reshape(token_count, query_heads, head_size)
    query_normed, query_back = jax.vjp(lambda inputs: head_norm(inputs, q_gain), query_raw)
    query_bf = query_normed.astype(jnp.bfloat16).reshape(
        token_count, kv_local, group_size, head_size
    )
    grad_bf = (
        (gate_value * d_out[0].astype(jnp.float32))
        .astype(jnp.bfloat16)
        .reshape(token_count, kv_local, group_size, head_size)
    )
    own_start = sequence_index * token_count
    all_queries = lax.all_gather(query_bf, "seq", axis=0, tiled=True)
    all_grads = lax.all_gather(grad_bf, "seq", axis=0, tiled=True)
    share_rows = tile_keys.shape[0]
    row_start = sequence_index * share_rows
    part_sum, part_weighted = attend_forward(
        all_queries, tile_keys, tile_values, seen_all, row_start, score_scale
    )
    all_weighted, all_weight_sum = (
        lax.psum(part_weighted.astype(jnp.bfloat16), "seq").astype(jnp.float32),
        lax.psum(part_sum.astype(jnp.bfloat16), "seq").astype(jnp.float32),
    )
    safe_all = jnp.where(all_weight_sum > 0, all_weight_sum, 1.0)
    context_all = all_weighted / jnp.transpose(safe_all, (2, 0, 1))[..., None]
    context = lax.dynamic_slice_in_dim(context_all, own_start, token_count, 0)
    row_delta = jnp.transpose(
        jnp.sum(all_grads.astype(jnp.float32) * context_all, axis=-1), (1, 2, 0)
    )
    grad_part, key_sums, value_sums = attend_backward(
        all_queries,
        all_grads,
        tile_keys,
        tile_values,
        seen_all,
        row_start,
        safe_all,
        row_delta,
        score_scale,
        token_count,
    )
    grad_query = lax.psum_scatter(
        grad_part.astype(jnp.bfloat16), "seq", scatter_dimension=0, tiled=True
    ).astype(jnp.float32)
    attended = (
        (gate_value * context).astype(jnp.bfloat16).reshape(1, token_count, query_heads * head_size)
    )
    key_round = key_sums.astype(jnp.bfloat16)
    value_round = value_sums.astype(jnp.bfloat16)
    back_keys = jnp.einsum(
        "to,rtf->orf", takes, key_round, preferred_element_type=jnp.float32
    ).astype(jnp.bfloat16)
    back_values = jnp.einsum(
        "to,rtf->orf", takes, value_round, preferred_element_type=jnp.float32
    ).astype(jnp.bfloat16)
    returned_keys, returned_values = (
        lax.all_to_all(
            lax.all_to_all(back_keys, "conv", split_axis=0, concat_axis=0, tiled=True),
            "tensor",
            split_axis=1,
            concat_axis=2,
            tiled=True,
        ),
        lax.all_to_all(
            lax.all_to_all(back_values, "conv", split_axis=0, concat_axis=0, tiled=True),
            "tensor",
            split_axis=1,
            concat_axis=2,
            tiled=True,
        ),
    )
    positioned_keys = jnp.einsum(
        "ew,eig->wig", transfers, returned_keys, preferred_element_type=jnp.float32
    )
    d_values = jnp.einsum(
        "ew,eig->wig", transfers, returned_values, preferred_element_type=jnp.float32
    ).astype(jnp.bfloat16)
    d_keys = key_back(positioned_keys.reshape(slot_count, row_local, kv_heads, head_size))[0]
    d_keys = d_keys.astype(jnp.bfloat16).reshape(slot_count, row_local, features)
    d_queries = query_back(grad_query.reshape(token_count, query_heads, head_size))[0]
    d_queries = d_queries.astype(jnp.bfloat16).reshape(1, token_count, query_heads * head_size)
    return (attended, d_queries, d_keys, d_values)


LOG2E = math.log2(math.e)


def inverse_rms(inputs):
    return lax.rsqrt(jnp.mean(inputs * inputs, axis=-1, keepdims=True) + EPSILON)


def norm_back(inputs, inv, gained):
    return inv * gained - inputs * (inv * inv * inv) * jnp.mean(
        inputs * gained, axis=-1, keepdims=True
    )


def dot(lhs, rhs):
    return jnp.dot(lhs, rhs, preferred_element_type=jnp.float32)


def head_kernel(
    owners, counts, gate, visible, q_gain_ref, k_gain_ref, q_hbm, do_hbm, k_hbm, v_hbm,
    att_hbm, dq_hbm, dk_hbm, dv_hbm,
    raw, sel, kvc, qa, da, seen, kn, kt, vt, wts, qs, qst, dt, acc, total, scaled_t, dos, delta,
    dqt, dk, dv, att_st, dq_st, grads, gsel,
    own_sem, conv_send, conv_recv, relay_send, relay_recv, kv_send, kv_recv,
    q_send, q_recv, own_q_sem, out_send, out_recv, own_out_sem,
    back_send, back_recv, backrelay_send, backrelay_recv, ret_send, ret_recv, own_ret_sem,
    *, conv_count, seq_count, tensor_count,
):
    c = lax.axis_index("conv")
    z = lax.axis_index("seq")
    x = lax.axis_index("tensor")
    tiles, row_local, features = k_hbm.shape
    size = q_gain_ref.shape[1]
    count = q_hbm.shape[0]
    width = qa.shape[2]
    lanes = qs.shape[1]
    group = width // size
    parts = seq_count * tensor_count
    heads_side = features // size // tensor_count
    scale = 1.0 / math.sqrt(size)

    def at(conv, seq, tensor):
        return {"conv": conv, "seq": seq, "tensor": tensor}

    def remote(src, dst, send, recv, device):
        return pltpu.make_async_remote_copy(
            src_ref=src, dst_ref=dst, send_sem=send, recv_sem=recv,
            device_id=device, device_id_type=pl.DeviceIdType.MESH,
        )

    def steps(j):
        return seq_count - 1 - j // tensor_count, tensor_count - 1 - j % tensor_count

    def target(j):
        k, e = steps(j)
        return lax.rem(z + k, seq_count), lax.rem(x + e, tensor_count)

    def source(j):
        k, e = steps(j)
        return lax.rem(z + seq_count - k, seq_count), lax.rem(x + tensor_count - e, tensor_count)

    def head_lanes(seq, tensor):
        return pl.ds(pl.multiple_of((tensor * heads_side + seq) * size, size), size)

    def group_lanes(seq):
        return pl.ds(pl.multiple_of(seq * width, width), width)

    partner = c + 1 - 2 * lax.rem(c, 2)
    siblings = [lax.rem(c + 2 * m, conv_count) for m in range(1, conv_count // 2)]
    fars = [lax.rem(partner + 2 * m, conv_count) for m in range(1, conv_count // 2)]
    others = [partner] + siblings
    own = parts - 1

    barrier = pltpu.get_barrier_semaphore()
    peers = [at(c, *target(j)) for j in range(own)] + [at(other, z, x) for other in others]
    for peer in peers:
        pl.semaphore_signal(barrier, inc=1, device_id=peer, device_id_type=pl.DeviceIdType.MESH)
    pl.semaphore_wait(barrier, len(peers))

    token_pairs = ((q_hbm, qa), (do_hbm, da))
    stores = (k_hbm, v_hbm)

    def q_copy(part, i):
        store, into = token_pairs[part]
        to = lax.rem(z + seq_count - i, seq_count)
        return remote(
            store.at[:, group_lanes(to)], into.at[z],
            q_send.at[part, i], q_recv.at[part, i], at(c, to, x),
        )

    def own_q_copy(part):
        store, into = token_pairs[part]
        return pltpu.make_async_copy(store.at[:, group_lanes(z)], into.at[z], own_q_sem.at[part])

    for i in range(1, seq_count):
        for part in range(2):
            q_copy(part, i).start()

    def raw_copy(j, part, n):
        src = stores[part].at[:, :, head_lanes(*target(j))]
        return remote(
            src, raw.at[c, j, part],
            conv_send.at[n, part, j], conv_recv.at[n, part, j], at(others[n], z, x),
        )

    def own_copy(j, part):
        src = stores[part].at[:, :, head_lanes(*target(j))]
        return pltpu.make_async_copy(src, raw.at[c, j, part], own_sem.at[part, j])

    @pl.loop(0, parts)
    def _(j):
        for n in reversed(range(len(others))):
            for part in range(2):
                raw_copy(j, part, n).start()
        for part in range(2):
            own_copy(j, part).start()

    for part in range(2):
        own_q_copy(part).start()

    seen_all = jnp.minimum(visible[pl.ds(c, 1), :], counts[c])
    for b in range(seq_count):
        piece = seen_all[:, b * count:(b + 1) * count]
        seen[b] = jnp.concatenate([piece] * group, axis=1)
    acc[...] = jnp.zeros_like(acc)
    total[...] = jnp.zeros_like(total)
    dqt[...] = jnp.zeros_like(dqt)
    q_gain = q_gain_ref[...]
    k_gain = k_gain_ref[...]
    gate_value = jnp.tanh(jnp.full((1, size), gate[0], jnp.float32))[:, :1]

    def relay(ref, j, m, send, recv):
        other = siblings[m]
        return remote(ref.at[other, j], ref.at[other, j], send.at[m, j], recv.at[m, j], at(partner, z, x))

    def relayed(ref, j, m, send, recv):
        return remote(ref.at[fars[m], j], ref.at[fars[m], j], send.at[m, j], recv.at[m, j], at(partner, z, x))

    def kv_copy(j):
        return remote(sel.at[j], kvc.at[j], kv_send.at[j], kv_recv.at[j], at(c, *target(j)))

    @pl.loop(0, parts)
    def _(j):
        for m, other in enumerate(siblings):
            came = len(siblings) - m
            for part in range(2):
                remote(
                    raw.at[other, j, part], raw.at[other, j, part],
                    conv_send.at[came, part, j], conv_recv.at[came, part, j], at(other, z, x),
                ).wait_recv()
            relay(raw, j, m, relay_send, relay_recv).start()
        for part in range(2):
            own_copy(j, part).wait()
            remote(
                raw.at[partner, j, part], raw.at[partner, j, part],
                conv_send.at[0, part, j], conv_recv.at[0, part, j], at(partner, z, x),
            ).wait_recv()
        for m in range(len(siblings)):
            relayed(raw, j, m, relay_send, relay_recv).wait_recv()
        for tile in range(tiles):
            for part in range(2):
                value = raw[0, j, part, tile]
                for conv in range(1, conv_count):
                    value = jnp.where(owners[tile, c] == conv, raw[conv, j, part, tile], value)
                sel[j, part, tile] = value

        @pl.when(j < own)
        def _():
            kv_copy(j).start()

    kvc[own] = sel[own]

    @pl.loop(0, seq_count)
    def _(i):
        block = lax.rem(z + i, seq_count)

        @pl.when(i == 0)
        def _():
            for part in range(2):
                own_q_copy(part).wait()

        @pl.when(i > 0)
        def _():
            for part, (store, into) in enumerate(token_pairs):
                remote(
                    store.at[:, group_lanes(z)], into.at[block],
                    q_send.at[part, i], q_recv.at[part, i], at(c, block, x),
                ).wait_recv()

        for g in range(group):
            piece = pl.ds(g * size, size)
            some = pl.ds(g * count, count)
            query = qa[block, :, piece].astype(jnp.float32)
            normed = query * inverse_rms(query) * (q_gain * (scale * LOG2E))
            qs[block, some, :] = normed.astype(jnp.bfloat16)
            qst[block, :, some] = normed.T.astype(jnp.bfloat16)
            dt[block, :, some] = (da[block, :, piece].astype(jnp.float32) * gate_value).T

    @pl.loop(0, parts)
    def _(n):
        j = lax.rem(n + parts - tensor_count, parts)

        @pl.when(j < own)
        def _():
            kv_copy(j).wait_recv()

        for tile in range(tiles):
            key = kvc[j, 0, tile].astype(jnp.float32)
            normed = key * inverse_rms(key) * k_gain
            kn[j, tile] = normed.astype(jnp.bfloat16)
            kt[j, tile] = normed.T.astype(jnp.bfloat16)
            vt[j, tile] = kvc[j, 1, tile].astype(jnp.float32).T.astype(jnp.bfloat16)
        from_seq, from_tensor = source(j)
        left = TILE - (from_seq * tensor_count + from_tensor) * row_local

        @pl.loop(0, seq_count)
        def _(b):
            seen_row = seen[b]
            part = jnp.zeros(acc.shape[1:], jnp.float32)
            part_sum = jnp.zeros(total.shape[1:], jnp.float32)
            for tile in range(tiles):
                limit = jnp.where(seen_row > tile, left, 0)
                w = jnp.exp2(dot(kn[j, tile], qst[b]))
                w = jnp.where(lax.broadcasted_iota(jnp.int32, w.shape, 0) < limit, w, 0.0)
                part_sum = part_sum + jnp.sum(w, axis=0, keepdims=True)
                w_bf = w.astype(jnp.bfloat16)
                wts[j, b, tile] = w_bf
                part = part + dot(vt[j, tile], w_bf)
            acc[b] += part
            total[b] += part_sum

    def out_copy(part, i):
        stage, out = ((att_st, att_hbm), (dq_st, dq_hbm))[part]
        to = lax.rem(z + i, seq_count)
        return remote(
            stage.at[to], out.at[:, group_lanes(z)],
            out_send.at[part, i], out_recv.at[part, seq_count - i], at(c, to, x),
        )

    def own_out_copy(part):
        stage, out = ((att_st, att_hbm), (dq_st, dq_hbm))[part]
        return pltpu.make_async_copy(stage.at[z], out.at[:, group_lanes(z)], own_out_sem.at[part])

    @pl.loop(0, seq_count)
    def _(n):
        b = lax.rem(z + n + 1, seq_count)
        inv = 1.0 / jnp.where(total[b] > 0, total[b], 1.0)
        ctx = acc[b] * inv
        for g in range(group):
            att_st[b, :, pl.ds(g * size, size)] = (
                (gate_value * ctx[:, g * count:(g + 1) * count]).T.astype(jnp.bfloat16)
            )
        scaled = (dt[b] * inv).astype(jnp.bfloat16)
        scaled32 = scaled.astype(jnp.float32)
        scaled_t[b] = scaled
        delta[b] = jnp.sum(scaled32 * ctx, axis=0, keepdims=True)

        @pl.when(n < seq_count - 1)
        def _():
            out_copy(0, n + 1).start()

        for g in range(group):
            dos[b, pl.ds(g * count, count), :] = (
                scaled32[:, g * count:(g + 1) * count].T.astype(jnp.bfloat16)
            )

    own_out_copy(0).start()

    def back_copy(j, n):
        return remote(
            grads.at[c, j], grads.at[c, j], back_send.at[n, j], back_recv.at[n, j],
            at(others[n], z, x),
        )

    def ret_copy(part, j):
        out = (dk_hbm, dv_hbm)[part]
        return remote(
            gsel.at[j, part], out.at[:, :, head_lanes(z, x)],
            ret_send.at[part, j], ret_recv.at[part, j], at(c, *source(j)),
        )

    def own_ret_copy(part):
        out = (dk_hbm, dv_hbm)[part]
        return pltpu.make_async_copy(
            gsel.at[own, part], out.at[:, :, head_lanes(z, x)], own_ret_sem.at[part]
        )

    def pass_back(j):
        for m, other in enumerate(siblings):
            came = len(siblings) - m
            remote(
                grads.at[other, j], grads.at[other, j], back_send.at[came, j],
                back_recv.at[came, j], at(other, z, x),
            ).wait_recv()
            relay(grads, j, m, backrelay_send, backrelay_recv).start()
        remote(
            grads.at[partner, j], grads.at[partner, j], back_send.at[0, j],
            back_recv.at[0, j], at(partner, z, x),
        ).wait_recv()
        for m in range(len(siblings)):
            relayed(grads, j, m, backrelay_send, backrelay_recv).wait_recv()
        for tile in range(tiles):
            for part in range(2):
                value = jnp.zeros((row_local, size), jnp.bfloat16)
                for conv in range(conv_count):
                    value = jnp.where(owners[tile, conv] == c, grads[conv, j, part, tile], value)
                gsel[j, part, tile] = value

        @pl.when(j < own)
        def _():
            for part in range(2):
                ret_copy(part, j).start()

    @pl.loop(0, parts)
    def _(j):
        dk[...] = jnp.zeros_like(dk)
        dv[...] = jnp.zeros_like(dv)

        @pl.loop(0, seq_count)
        def _(b):
            low = delta[b]
            part = jnp.zeros(dqt.shape[1:], jnp.float32)
            for tile in range(tiles):
                w_bf = wts[j, b, tile]
                dp = dot(kvc[j, 1, tile], scaled_t[b])
                ds = (w_bf.astype(jnp.float32) * (dp - low)).astype(jnp.bfloat16)
                dv[tile] += dot(w_bf, dos[b])
                dk[tile] += dot(ds, qs[b])
                part = part + dot(kt[j, tile], ds)
            dqt[b] += part

        for tile in range(tiles):
            key = kvc[j, 0, tile].astype(jnp.float32)
            grad = dk[tile] * (1.0 / LOG2E) * k_gain
            grads[c, j, 0, tile] = norm_back(key, inverse_rms(key), grad).astype(jnp.bfloat16)
            grads[c, j, 1, tile] = dv[tile].astype(jnp.bfloat16)
        for n in reversed(range(len(others))):
            back_copy(j, n).start()

        @pl.when(j == parts // 2)
        def _():
            pass_back(0)

    @pl.loop(0, seq_count)
    def _(n):
        b = lax.rem(z + n + 1, seq_count)
        for g in range(group):
            piece = pl.ds(g * size, size)
            query = qa[b, :, piece].astype(jnp.float32)
            grad = dqt[b, :, pl.ds(g * count, count)].T * (q_gain * scale)
            dq_st[b, :, piece] = norm_back(query, inverse_rms(query), grad).astype(jnp.bfloat16)

        @pl.when(n < seq_count - 1)
        def _():
            out_copy(1, n + 1).start()

    own_out_copy(1).start()

    @pl.loop(1, parts)
    def _(j):
        pass_back(j)

    for part in range(2):
        own_ret_copy(part).start()

    @pl.loop(0, parts)
    def _(j):
        for n in range(len(others)):
            for part in range(2):
                raw_copy(j, part, n).wait_send()
            back_copy(j, n).wait_send()
        for m in range(len(siblings)):
            relay(raw, j, m, relay_send, relay_recv).wait_send()
            relay(grads, j, m, backrelay_send, backrelay_recv).wait_send()

    @pl.loop(0, own)
    def _(j):
        kv_copy(j).wait_send()
        for part in range(2):
            ret_copy(part, j).wait_send()
            out = (dk_hbm, dv_hbm)[part]
            remote(
                gsel.at[j, part], out.at[:, :, head_lanes(*target(j))],
                ret_send.at[part, j], ret_recv.at[part, j], at(c, *target(j)),
            ).wait_recv()

    for part, (stage, out) in enumerate(((att_st, att_hbm), (dq_st, dq_hbm))):
        for i in range(1, seq_count):
            q_copy(part, i).wait_send()
            came = lax.rem(z + seq_count - i, seq_count)
            remote(
                stage.at[came], out.at[:, group_lanes(lax.rem(z + i, seq_count))],
                out_send.at[part, i], out_recv.at[part, i], at(c, came, x),
            ).wait()
        own_out_copy(part).wait()
        own_ret_copy(part).wait()


def head_shards(queries, keys, values, q_gain, k_gain, gate, tile_count, tile_owner, visible, d_out):
    conv_count = lax.axis_size("conv")
    tensor_count = lax.axis_size("tensor")
    seq_count = lax.axis_size("seq")
    tiles, row_local, features = keys.shape
    size = q_gain.shape[0]
    count, width_all = queries.shape[1:]
    width = width_all // seq_count
    lanes = width // size * count
    bf, f32 = jnp.bfloat16, jnp.float32
    parts = seq_count * tensor_count
    far = conv_count // 2 - 1
    chunk = (2, tiles, row_local, size)
    v, dma = pltpu.VMEM, pltpu.SemaphoreType.DMA

    vmem = pl.BlockSpec(memory_space=pltpu.VMEM)
    smem = pl.BlockSpec(memory_space=pltpu.SMEM)
    hbm = pl.BlockSpec(memory_space=pl.ANY)
    att, dq, dk, dv = pl.pallas_call(
        partial(
            head_kernel, conv_count=conv_count, seq_count=seq_count, tensor_count=tensor_count
        ),
        out_shape=[jax.ShapeDtypeStruct((count, width_all), bf)] * 2
        + [jax.ShapeDtypeStruct(keys.shape, bf)] * 2,
        in_specs=[smem] * 3 + [vmem] * 3 + [hbm] * 4,
        out_specs=[hbm] * 4,
        scratch_shapes=[
            v((conv_count, parts) + chunk, bf),
            v((parts,) + chunk, bf),
            v((parts,) + chunk, bf),
            v((seq_count, count, width), bf),
            v((seq_count, count, width), bf),
            v((seq_count, 1, lanes), jnp.int32),
            v((parts, tiles, row_local, size), bf),
            v((parts, tiles, size, row_local), bf),
            v((parts, tiles, size, row_local), bf),
            v((parts, seq_count, tiles, row_local, lanes), bf),
            v((seq_count, lanes, size), bf),
            v((seq_count, size, lanes), bf),
            v((seq_count, size, lanes), f32),
            v((seq_count, size, lanes), f32),
            v((seq_count, 1, lanes), f32),
            v((seq_count, size, lanes), bf),
            v((seq_count, lanes, size), bf),
            v((seq_count, 1, lanes), f32),
            v((seq_count, size, lanes), f32),
            v((tiles, row_local, size), f32),
            v((tiles, row_local, size), f32),
            v((seq_count, count, width), bf),
            v((seq_count, count, width), bf),
            v((conv_count, parts) + chunk, bf),
            v((parts,) + chunk, bf),
            dma((2, parts)), dma((far + 1, 2, parts)), dma((far + 1, 2, parts)),
            dma((far, parts)), dma((far, parts)), dma((parts,)), dma((parts,)),
            dma((2, seq_count)), dma((2, seq_count)), dma((2,)),
            dma((2, seq_count)), dma((2, seq_count)), dma((2,)),
            dma((far + 1, parts)), dma((far + 1, parts)), dma((far, parts)), dma((far, parts)),
            dma((2, parts)), dma((2, parts)), dma((2,)),
        ],
        compiler_params=pltpu.CompilerParams(
            collective_id=0, has_side_effects=True, vmem_limit_bytes=60 << 20
        ),
    )(
        tile_owner.T, tile_count, gate, visible, q_gain[None], k_gain[None],
        queries[0], d_out[0], keys, values,
    )
    return (att[None], dq[None], dk, dv)


def shards(queries, keys, *rest):
    heads = keys.shape[2] // rest[1].shape[0]
    seq_count, tensor_count = lax.axis_size("seq"), lax.axis_size("tensor")
    conv_count = lax.axis_size("conv")
    fits = heads == seq_count * tensor_count and conv_count % 2 == 0 and conv_count > 2
    fits = fits and keys.shape[1] % 16 == 0
    return (head_shards if fits else row_shards)(queries, keys, *rest)


def solution(mesh):
    in_specs = (
        P("conv", "seq", "tensor"),
        P("conv", ("seq", "tensor"), None),
        P("conv", ("seq", "tensor"), None),
        P(),
        P(),
        P(),
        P(),
        P(),
        P(),
        P("conv", "seq", "tensor"),
    )
    out_specs = (
        P("conv", "seq", "tensor"),
        P("conv", "seq", "tensor"),
        P("conv", ("seq", "tensor"), None),
        P("conv", ("seq", "tensor"), None),
    )
    return jax.shard_map(shards, mesh=mesh, in_specs=in_specs, out_specs=out_specs, check_vma=False)
```

```python
from functools import partial
import math

import jax
import jax.numpy as jnp
from jax import lax
from jax.experimental import pallas as pl
from jax.experimental.pallas import tpu as pltpu
from jax.sharding import PartitionSpec as P

TILE = 1601


EPSILON = 1e-05


def head_norm(inputs, norm_gain):
    mean_square = jnp.mean(inputs * inputs, axis=-1, keepdims=True)
    return inputs * lax.rsqrt(mean_square + EPSILON) * norm_gain


def key_mask(seen_tiles, tile_index, row_start, row_count):
    row_ids = row_start + jnp.arange(row_count, dtype=jnp.int32)
    return (seen_tiles > tile_index)[:, None] & (row_ids < TILE)[None, :]


def tile_weights(query_bf, key_tile, visible_keys, score_scale):
    scores = (
        jnp.einsum("pkgd,rkd->kgpr", query_bf, key_tile, preferred_element_type=jnp.float32)
        * score_scale
    )
    return jnp.where(visible_keys[None, None], jnp.exp(scores), 0.0)


def tile_forward(query_bf, key_tile, value_tile, visible_keys, score_scale):
    weights = tile_weights(query_bf, key_tile, visible_keys, score_scale)
    weighted = jnp.einsum(
        "kgpr,rkd->pkgd",
        weights.astype(jnp.bfloat16),
        value_tile,
        preferred_element_type=jnp.float32,
    )
    return (jnp.sum(weights, axis=-1), weighted)


def tile_gradients(
    query_bf,
    grad_bf,
    key_tile,
    value_tile,
    visible_keys,
    safe_sum,
    row_delta,
    score_scale,
    block_count,
):
    weights = tile_weights(query_bf, key_tile, visible_keys, score_scale)
    probability = weights / safe_sum[..., None]
    grad_prob = jnp.einsum(
        "pkgd,rkd->kgpr", grad_bf, value_tile, preferred_element_type=jnp.float32
    )
    grad_score = (probability * (grad_prob - row_delta[..., None])).astype(jnp.bfloat16)
    prob_bf = probability.astype(jnp.bfloat16)
    grad_query = (
        jnp.einsum("kgpr,rkd->pkgd", grad_score, key_tile, preferred_element_type=jnp.float32)
        * score_scale
    )
    kv_local, group_size, token_count, row_count = grad_score.shape
    head_size = query_bf.shape[-1]
    block_tokens = token_count // block_count
    score_blocks = grad_score.reshape(kv_local, group_size, block_count, block_tokens, row_count)
    prob_blocks = prob_bf.reshape(kv_local, group_size, block_count, block_tokens, row_count)
    query_blocks = query_bf.reshape(block_count, block_tokens, kv_local, group_size, head_size)
    grad_blocks = grad_bf.reshape(block_count, block_tokens, kv_local, group_size, head_size)
    key_part = (
        jnp.einsum(
            "kgbpr,bpkgd->brkd", score_blocks, query_blocks, preferred_element_type=jnp.float32
        )
        * score_scale
    )
    value_part = jnp.einsum(
        "kgbpr,bpkgd->brkd", prob_blocks, grad_blocks, preferred_element_type=jnp.float32
    )
    key_part = jnp.sum(
        lax.optimization_barrier(key_part.astype(jnp.bfloat16)).astype(jnp.float32), axis=0
    )
    value_part = jnp.sum(
        lax.optimization_barrier(value_part.astype(jnp.bfloat16)).astype(jnp.float32), axis=0
    )
    return (
        grad_query,
        key_part.reshape(row_count, kv_local * head_size),
        value_part.reshape(row_count, kv_local * head_size),
    )


def attend_forward(query_bf, tile_keys, tile_values, seen_tiles, row_start, score_scale):
    row_count, slot_count, features = tile_keys.shape
    token_count, kv_local, group_size, head_size = query_bf.shape
    weight_sum = jnp.zeros((kv_local, group_size, token_count), jnp.float32)
    weighted = jnp.zeros(query_bf.shape, jnp.float32)
    for tile_index in range(slot_count):
        key_tile = tile_keys[:, tile_index].reshape(row_count, kv_local, head_size)
        value_tile = tile_values[:, tile_index].reshape(row_count, kv_local, head_size)
        visible_keys = key_mask(seen_tiles, tile_index, row_start, row_count)
        work = partial(tile_forward, query_bf, key_tile, value_tile, visible_keys, score_scale)
        part_sum, part_weighted = work()
        weight_sum = weight_sum + part_sum
        weighted = weighted + part_weighted
    return (weight_sum, weighted)


def attend_backward(
    query_bf,
    grad_bf,
    tile_keys,
    tile_values,
    seen_tiles,
    row_start,
    safe_sum,
    row_delta,
    score_scale,
    block_tokens,
):
    row_count, slot_count, features = tile_keys.shape
    token_count, kv_local, group_size, head_size = query_bf.shape
    block_count = token_count // block_tokens
    grad_query = jnp.zeros(query_bf.shape, jnp.float32)
    key_parts = []
    value_parts = []
    for tile_index in range(slot_count):
        key_tile = tile_keys[:, tile_index].reshape(row_count, kv_local, head_size)
        value_tile = tile_values[:, tile_index].reshape(row_count, kv_local, head_size)
        visible_keys = key_mask(seen_tiles, tile_index, row_start, row_count)
        work = partial(
            tile_gradients,
            query_bf,
            grad_bf,
            key_tile,
            value_tile,
            visible_keys,
            safe_sum,
            row_delta,
            score_scale,
            block_count,
        )
        part_query, key_part, value_part = work()
        grad_query = grad_query + part_query
        key_parts.append(key_part)
        value_parts.append(value_part)
    return (grad_query, jnp.stack(key_parts, axis=1), jnp.stack(value_parts, axis=1))


def row_shards(queries, keys, values, q_gain, k_gain, gate, tile_count, tile_owner, visible, d_out):
    conv_count = lax.axis_size("conv")
    tensor_count = lax.axis_size("tensor")
    conv_index = lax.axis_index("conv")
    sequence_index = lax.axis_index("seq")
    slot_count, row_local, features = keys.shape
    head_size = q_gain.shape[0]
    kv_heads = features // head_size
    kv_local = kv_heads // tensor_count
    token_count = queries.shape[1]
    query_heads = queries.shape[2] // head_size
    group_size = query_heads // kv_local
    score_scale = 1.0 / math.sqrt(head_size)
    gate_value = jnp.tanh(gate[0])
    conv_ids = jnp.arange(conv_count, dtype=jnp.int32)
    transfers = (tile_owner == conv_index).astype(jnp.bfloat16)
    own_owners = lax.dynamic_index_in_dim(tile_owner, conv_index, 0, keepdims=False)
    takes = (own_owners[:, None] == conv_ids[None, :]).astype(jnp.bfloat16)
    own_count = lax.dynamic_index_in_dim(tile_count, conv_index, 0, keepdims=False)
    seen_all = jnp.minimum(
        lax.dynamic_index_in_dim(visible, conv_index, 0, keepdims=False), own_count
    )
    key_raw = keys.astype(jnp.float32).reshape(slot_count, row_local, kv_heads, head_size)
    key_normed, key_back = jax.vjp(lambda inputs: head_norm(inputs, k_gain), key_raw)
    key_halfprec = key_normed.astype(jnp.bfloat16).reshape(slot_count, row_local, features)
    outgoing_keys = jnp.einsum(
        "wn,nki->wki", transfers, key_halfprec, preferred_element_type=jnp.float32
    ).astype(jnp.bfloat16)
    send_values = jnp.einsum(
        "wn,nki->wki", transfers, values, preferred_element_type=jnp.float32
    ).astype(jnp.bfloat16)
    got_keys, got_values = (
        lax.all_to_all(
            lax.all_to_all(outgoing_keys, "conv", split_axis=0, concat_axis=0, tiled=True),
            "tensor",
            split_axis=2,
            concat_axis=1,
            tiled=True,
        ),
        lax.all_to_all(
            lax.all_to_all(send_values, "conv", split_axis=0, concat_axis=0, tiled=True),
            "tensor",
            split_axis=2,
            concat_axis=1,
            tiled=True,
        ),
    )
    tile_keys = jnp.einsum(
        "to,orf->rtf", takes, got_keys, preferred_element_type=jnp.float32
    ).astype(jnp.bfloat16)
    tile_values = jnp.einsum(
        "to,orf->rtf", takes, got_values, preferred_element_type=jnp.float32
    ).astype(jnp.bfloat16)
    query_raw = queries[0].astype(jnp.float32).reshape(token_count, query_heads, head_size)
    query_normed, query_back = jax.vjp(lambda inputs: head_norm(inputs, q_gain), query_raw)
    query_bf = query_normed.astype(jnp.bfloat16).reshape(
        token_count, kv_local, group_size, head_size
    )
    grad_bf = (
        (gate_value * d_out[0].astype(jnp.float32))
        .astype(jnp.bfloat16)
        .reshape(token_count, kv_local, group_size, head_size)
    )
    own_start = sequence_index * token_count
    all_queries = lax.all_gather(query_bf, "seq", axis=0, tiled=True)
    all_grads = lax.all_gather(grad_bf, "seq", axis=0, tiled=True)
    share_rows = tile_keys.shape[0]
    row_start = sequence_index * share_rows
    part_sum, part_weighted = attend_forward(
        all_queries, tile_keys, tile_values, seen_all, row_start, score_scale
    )
    all_weighted, all_weight_sum = (
        lax.psum(part_weighted.astype(jnp.bfloat16), "seq").astype(jnp.float32),
        lax.psum(part_sum.astype(jnp.bfloat16), "seq").astype(jnp.float32),
    )
    safe_all = jnp.where(all_weight_sum > 0, all_weight_sum, 1.0)
    context_all = all_weighted / jnp.transpose(safe_all, (2, 0, 1))[..., None]
    context = lax.dynamic_slice_in_dim(context_all, own_start, token_count, 0)
    row_delta = jnp.transpose(
        jnp.sum(all_grads.astype(jnp.float32) * context_all, axis=-1), (1, 2, 0)
    )
    grad_part, key_sums, value_sums = attend_backward(
        all_queries,
        all_grads,
        tile_keys,
        tile_values,
        seen_all,
        row_start,
        safe_all,
        row_delta,
        score_scale,
        token_count,
    )
    grad_query = lax.psum_scatter(
        grad_part.astype(jnp.bfloat16), "seq", scatter_dimension=0, tiled=True
    ).astype(jnp.float32)
    attended = (
        (gate_value * context).astype(jnp.bfloat16).reshape(1, token_count, query_heads * head_size)
    )
    key_round = key_sums.astype(jnp.bfloat16)
    value_round = value_sums.astype(jnp.bfloat16)
    back_keys = jnp.einsum(
        "to,rtf->orf", takes, key_round, preferred_element_type=jnp.float32
    ).astype(jnp.bfloat16)
    back_values = jnp.einsum(
        "to,rtf->orf", takes, value_round, preferred_element_type=jnp.float32
    ).astype(jnp.bfloat16)
    returned_keys, returned_values = (
        lax.all_to_all(
            lax.all_to_all(back_keys, "conv", split_axis=0, concat_axis=0, tiled=True),
            "tensor",
            split_axis=1,
            concat_axis=2,
            tiled=True,
        ),
        lax.all_to_all(
            lax.all_to_all(back_values, "conv", split_axis=0, concat_axis=0, tiled=True),
            "tensor",
            split_axis=1,
            concat_axis=2,
            tiled=True,
        ),
    )
    positioned_keys = jnp.einsum(
        "ew,eig->wig", transfers, returned_keys, preferred_element_type=jnp.float32
    )
    d_values = jnp.einsum(
        "ew,eig->wig", transfers, returned_values, preferred_element_type=jnp.float32
    ).astype(jnp.bfloat16)
    d_keys = key_back(positioned_keys.reshape(slot_count, row_local, kv_heads, head_size))[0]
    d_keys = d_keys.astype(jnp.bfloat16).reshape(slot_count, row_local, features)
    d_queries = query_back(grad_query.reshape(token_count, query_heads, head_size))[0]
    d_queries = d_queries.astype(jnp.bfloat16).reshape(1, token_count, query_heads * head_size)
    return (attended, d_queries, d_keys, d_values)


LOG2E = math.log2(math.e)


def inverse_rms(inputs):
    return lax.rsqrt(jnp.mean(inputs * inputs, axis=-1, keepdims=True) + EPSILON)


def norm_back(inputs, inv, gained):
    return inv * gained - inputs * (inv * inv * inv) * jnp.mean(
        inputs * gained, axis=-1, keepdims=True
    )


def dot(lhs, rhs):
    return jnp.dot(lhs, rhs, preferred_element_type=jnp.float32)


def head_kernel(
    owners, counts, gate, visible, q_gain_ref, k_gain_ref, q_hbm, do_hbm, k_hbm, v_hbm,
    att_hbm, dq_hbm, dk_hbm, dv_hbm,
    raw, sel, kvc, qa, da, seen, kn, kt, vt, wts, qs, qst, dt, acc, total, scaled_t, dos, delta,
    dqt, dss, att_st, dq_st, grads, gsel,
    own_sem, conv_send, conv_recv, relay_send, relay_recv, kv_send, kv_recv,
    q_send, q_recv, own_q_sem, out_send, out_recv, own_out_sem,
    back_send, back_recv, backrelay_send, backrelay_recv, ret_send, ret_recv, own_ret_sem,
    *, conv_count, seq_count, tensor_count,
):
    c = lax.axis_index("conv")
    z = lax.axis_index("seq")
    x = lax.axis_index("tensor")
    tiles, row_local, features = k_hbm.shape
    size = q_gain_ref.shape[1]
    count = q_hbm.shape[0]
    width = qa.shape[2]
    group = width // size
    lanes = group * count
    parts = seq_count * tensor_count
    rows = tiles * row_local
    heads_side = features // size // tensor_count
    scale = 1.0 / math.sqrt(size)

    def at(conv, seq, tensor):
        return {"conv": conv, "seq": seq, "tensor": tensor}

    def remote(src, dst, send, recv, device):
        return pltpu.make_async_remote_copy(
            src_ref=src, dst_ref=dst, send_sem=send, recv_sem=recv,
            device_id=device, device_id_type=pl.DeviceIdType.MESH,
        )

    def steps(j):
        return seq_count - 1 - j // tensor_count, tensor_count - 1 - j % tensor_count

    half = z // (seq_count // 2)

    def hop(q):
        k = 1 + (q + seq_count // 2 + seq_count - 3) % (seq_count - 1)
        k = (q + seq_count - 1) // seq_count * k
        return lax.rem(k + half * (seq_count - 2 * k), seq_count)

    def place(k, n):
        return (seq_count - 1 - k) * tensor_count + n % tensor_count

    def send_order(n):
        return place(hop(n // tensor_count), n)

    def back_order(n):
        n = lax.rem(n + tensor_count, parts)
        return place(lax.rem(seq_count - hop(n // tensor_count), seq_count), n)

    def target(j):
        k, e = steps(j)
        return lax.rem(z + k, seq_count), lax.rem(x + e, tensor_count)

    def source(j):
        k, e = steps(j)
        return lax.rem(z + seq_count - k, seq_count), lax.rem(x + tensor_count - e, tensor_count)

    def head_lanes(seq, tensor):
        return pl.ds(pl.multiple_of((tensor * heads_side + seq) * size, size), size)

    def block_lanes(b, start=0, length=lanes):
        return pl.ds(pl.multiple_of(b * lanes + start, size), length)

    def group_lanes(seq):
        return pl.ds(pl.multiple_of(seq * width, width), width)

    partner = c + 1 - 2 * lax.rem(c, 2)
    siblings = [lax.rem(c + 2 * m, conv_count) for m in range(1, conv_count // 2)]
    fars = [lax.rem(partner + 2 * m, conv_count) for m in range(1, conv_count // 2)]
    others = [partner] + siblings
    own = parts - 1

    barrier = pltpu.get_barrier_semaphore()
    peers = [at(c, *target(j)) for j in range(own)] + [at(other, z, x) for other in others]
    for peer in peers:
        pl.semaphore_signal(barrier, inc=1, device_id=peer, device_id_type=pl.DeviceIdType.MESH)
    pl.semaphore_wait(barrier, len(peers))

    token_pairs = ((q_hbm, qa), (do_hbm, da))
    stores = (k_hbm, v_hbm)

    def q_copy(part, i):
        store, into = token_pairs[part]
        to = lax.rem(z + seq_count - i, seq_count)
        return remote(
            store.at[:, group_lanes(to)], into.at[z],
            q_send.at[part, i], q_recv.at[part, i], at(c, to, x),
        )

    def own_q_copy(part):
        store, into = token_pairs[part]
        return pltpu.make_async_copy(store.at[:, group_lanes(z)], into.at[z], own_q_sem.at[part])

    @pl.loop(1, seq_count)
    def _(q):
        for part in range(2):
            q_copy(part, seq_count - hop(q)).start()

    def raw_copy(j, part, n):
        src = stores[part].at[:, :, head_lanes(*target(j))]
        return remote(
            src, raw.at[c, j, part],
            conv_send.at[n, part, j], conv_recv.at[n, part, j], at(others[n], z, x),
        )

    def own_copy(j, part):
        src = stores[part].at[:, :, head_lanes(*target(j))]
        return pltpu.make_async_copy(src, raw.at[c, j, part], own_sem.at[part, j])

    @pl.loop(0, parts)
    def _(step):
        j = send_order(step)
        for n in reversed(range(len(others))):
            for part in range(2):
                raw_copy(j, part, n).start()
        for part in range(2):
            own_copy(j, part).start()

    for part in range(2):
        own_q_copy(part).start()

    seen_all = jnp.minimum(visible[pl.ds(c, 1), :], counts[c])
    for b in range(seq_count):
        piece = seen_all[:, b * count:(b + 1) * count]
        seen[b] = jnp.concatenate([piece] * group, axis=1)
    acc[...] = jnp.zeros_like(acc)
    total[...] = jnp.zeros_like(total)
    dqt[...] = jnp.zeros_like(dqt)
    q_gain = q_gain_ref[...]
    k_gain = k_gain_ref[...]
    gate_value = jnp.tanh(jnp.full((1, size), gate[0], jnp.float32))[:, :1]

    def relay(ref, j, m, send, recv):
        other = siblings[m]
        return remote(ref.at[other, j], ref.at[other, j], send.at[m, j], recv.at[m, j], at(partner, z, x))

    def relayed(ref, j, m, send, recv):
        return remote(ref.at[fars[m], j], ref.at[fars[m], j], send.at[m, j], recv.at[m, j], at(partner, z, x))

    def kv_copy(j):
        return remote(sel.at[j], kvc.at[j], kv_send.at[j], kv_recv.at[j], at(c, *target(j)))

    def take_tokens(q):
        i = lax.rem(seq_count - hop(q), seq_count)
        block = lax.rem(z + i, seq_count)

        @pl.when(q == 0)
        def _():
            for part in range(2):
                own_q_copy(part).wait()

        @pl.when(q > 0)
        def _():
            for part, (store, into) in enumerate(token_pairs):
                remote(
                    store.at[:, group_lanes(z)], into.at[block],
                    q_send.at[part, i], q_recv.at[part, i], at(c, block, x),
                ).wait_recv()

        for g in range(group):
            piece = pl.ds(g * size, size)
            some = block_lanes(block, g * count, count)
            query = qa[block, :, piece].astype(jnp.float32)
            normed = query * inverse_rms(query) * (q_gain * (scale * LOG2E))
            qs[some, :] = normed.astype(jnp.bfloat16)
            qst[:, some] = normed.T.astype(jnp.bfloat16)
            dt[:, some] = (da[block, :, piece].astype(jnp.float32) * gate_value).T

    @pl.loop(0, parts)
    def _(step):
        j = send_order(step)
        for m, other in enumerate(siblings):
            came = len(siblings) - m
            for part in range(2):
                remote(
                    raw.at[other, j, part], raw.at[other, j, part],
                    conv_send.at[came, part, j], conv_recv.at[came, part, j], at(other, z, x),
                ).wait_recv()
            relay(raw, j, m, relay_send, relay_recv).start()
        for part in range(2):
            own_copy(j, part).wait()
            remote(
                raw.at[partner, j, part], raw.at[partner, j, part],
                conv_send.at[0, part, j], conv_recv.at[0, part, j], at(partner, z, x),
            ).wait_recv()
        for m in range(len(siblings)):
            relayed(raw, j, m, relay_send, relay_recv).wait_recv()
        for tile in range(tiles):
            for part in range(2):
                value = raw[0, j, part, tile]
                for conv in range(1, conv_count):
                    value = jnp.where(owners[tile, c] == conv, raw[conv, j, part, tile], value)
                sel[j, part, tile] = value

        @pl.when(j < own)
        def _():
            kv_copy(j).start()

        @pl.when(step >= parts - seq_count)
        def _():
            take_tokens(step - (parts - seq_count))

    kvc[own] = sel[own]

    @pl.loop(0, parts)
    def _(n):
        j = send_order(n)

        @pl.when(j < own)
        def _():
            kv_copy(j).wait_recv()

        key = kvc[j, 0].reshape(rows, size).astype(jnp.float32)
        normed = key * inverse_rms(key) * k_gain
        kn[j] = normed.astype(jnp.bfloat16)
        kt[j] = normed.T.astype(jnp.bfloat16)
        vt[j] = kvc[j, 1].reshape(rows, size).astype(jnp.float32).T.astype(jnp.bfloat16)
        from_seq, from_tensor = source(j)
        left = TILE - (from_seq * tensor_count + from_tensor) * row_local

        for b in range(seq_count):
            some = pl.ds(b * lanes, lanes)
            seen_row = seen[b]
            scores = dot(kn[j], qst[:, some])
            part_sum = jnp.zeros((1, lanes), jnp.float32)
            for tile in range(tiles):
                limit = jnp.where(seen_row > tile, left, 0)
                w = jnp.exp2(scores[tile * row_local:(tile + 1) * row_local])
                w = jnp.where(lax.broadcasted_iota(jnp.int32, w.shape, 0) < limit, w, 0.0)
                part_sum = part_sum + jnp.sum(w, axis=0, keepdims=True)
                wts[j, pl.ds(tile * row_local, row_local), some] = w.astype(jnp.bfloat16)
            total[:, some] += part_sum
        for b in range(seq_count):
            some = pl.ds(b * lanes, lanes)
            acc[:, some] += dot(vt[j], wts[j, :, some])

    def out_copy(part, i):
        stage, out = ((att_st, att_hbm), (dq_st, dq_hbm))[part]
        to = lax.rem(z + i, seq_count)
        return remote(
            stage.at[to], out.at[:, group_lanes(z)],
            out_send.at[part, i], out_recv.at[part, seq_count - i], at(c, to, x),
        )

    def own_out_copy(part):
        stage, out = ((att_st, att_hbm), (dq_st, dq_hbm))[part]
        return pltpu.make_async_copy(stage.at[z], out.at[:, group_lanes(z)], own_out_sem.at[part])

    @pl.loop(0, seq_count)
    def _(n):
        i = hop(lax.rem(n + 1, seq_count))
        b = lax.rem(z + i, seq_count)
        some = block_lanes(b)
        sums = total[:, some]
        inv = 1.0 / jnp.where(sums > 0, sums, 1.0)
        ctx = acc[:, some] * inv
        for g in range(group):
            att_st[b, :, pl.ds(g * size, size)] = (
                (gate_value * ctx[:, g * count:(g + 1) * count]).T.astype(jnp.bfloat16)
            )
        scaled = (dt[:, some] * inv).astype(jnp.bfloat16)
        scaled32 = scaled.astype(jnp.float32)
        scaled_t[:, some] = scaled
        delta[:, some] = jnp.sum(scaled32 * ctx, axis=0, keepdims=True)

        @pl.when(n < seq_count - 1)
        def _():
            out_copy(0, i).start()

        for g in range(group):
            dos[block_lanes(b, g * count, count), :] = (
                scaled32[:, g * count:(g + 1) * count].T.astype(jnp.bfloat16)
            )

    own_out_copy(0).start()

    def back_copy(j, n):
        return remote(
            grads.at[c, j], grads.at[c, j], back_send.at[n, j], back_recv.at[n, j],
            at(others[n], z, x),
        )

    def ret_copy(part, j):
        out = (dk_hbm, dv_hbm)[part]
        return remote(
            gsel.at[j, part], out.at[:, :, head_lanes(z, x)],
            ret_send.at[part, j], ret_recv.at[part, j], at(c, *source(j)),
        )

    def own_ret_copy(part):
        out = (dk_hbm, dv_hbm)[part]
        return pltpu.make_async_copy(
            gsel.at[own, part], out.at[:, :, head_lanes(z, x)], own_ret_sem.at[part]
        )

    def pass_back(n):
        j = back_order(n)
        for m, other in enumerate(siblings):
            came = len(siblings) - m
            remote(
                grads.at[other, j], grads.at[other, j], back_send.at[came, j],
                back_recv.at[came, j], at(other, z, x),
            ).wait_recv()
            relay(grads, j, m, backrelay_send, backrelay_recv).start()
        remote(
            grads.at[partner, j], grads.at[partner, j], back_send.at[0, j],
            back_recv.at[0, j], at(partner, z, x),
        ).wait_recv()
        for m in range(len(siblings)):
            relayed(grads, j, m, backrelay_send, backrelay_recv).wait_recv()
        for tile in range(tiles):
            for part in range(2):
                value = jnp.zeros((row_local, size), jnp.bfloat16)
                for conv in range(conv_count):
                    value = jnp.where(owners[tile, conv] == c, grads[conv, j, part, tile], value)
                gsel[j, part, tile] = value

        @pl.when(j < own)
        def _():
            for part in range(2):
                ret_copy(part, j).start()

    @pl.loop(0, parts)
    def _(n):
        j = back_order(n)
        value = kvc[j, 1].reshape(rows, size)
        for b in range(seq_count):
            some = pl.ds(b * lanes, lanes)
            dp = dot(value, scaled_t[:, some])
            score = wts[j, :, some].astype(jnp.float32) * (dp - delta[:, some])
            dss[:, some] = score.astype(jnp.bfloat16)
        dv = dot(wts[j], dos[...])
        dk = dot(dss[...], qs[...])
        for b in range(seq_count):
            some = pl.ds(b * lanes, lanes)
            dqt[:, some] += dot(kt[j], dss[:, some])

        key = kvc[j, 0].reshape(rows, size).astype(jnp.float32)
        grad = dk * (1.0 / LOG2E) * k_gain
        grad = norm_back(key, inverse_rms(key), grad).astype(jnp.bfloat16)
        grads[c, j, 0] = grad.reshape(tiles, row_local, size)
        grads[c, j, 1] = dv.astype(jnp.bfloat16).reshape(tiles, row_local, size)
        for m in reversed(range(len(others))):
            back_copy(j, m).start()

        late = n - parts // 2

        @pl.when((late >= 0) & (late % 2 == 0))
        def _():
            pass_back(late // 2)

    passed = (parts - parts // 2 + 1) // 2
    pass_back(passed)

    @pl.loop(0, seq_count)
    def _(n):
        i = hop(lax.rem(n + 1, seq_count))
        b = lax.rem(z + i, seq_count)
        for g in range(group):
            piece = pl.ds(g * size, size)
            query = qa[b, :, piece].astype(jnp.float32)
            grad = dqt[:, block_lanes(b, g * count, count)].T * (q_gain * scale)
            dq_st[b, :, piece] = norm_back(query, inverse_rms(query), grad).astype(jnp.bfloat16)

        @pl.when(n < seq_count - 1)
        def _():
            out_copy(1, i).start()

    own_out_copy(1).start()

    @pl.loop(passed + 1, parts)
    def _(n):
        pass_back(n)

    for part in range(2):
        own_ret_copy(part).start()

    @pl.loop(0, parts)
    def _(j):
        for n in range(len(others)):
            for part in range(2):
                raw_copy(j, part, n).wait_send()
            back_copy(j, n).wait_send()
        for m in range(len(siblings)):
            relay(raw, j, m, relay_send, relay_recv).wait_send()
            relay(grads, j, m, backrelay_send, backrelay_recv).wait_send()

    @pl.loop(0, own)
    def _(j):
        kv_copy(j).wait_send()
        for part in range(2):
            ret_copy(part, j).wait_send()
            out = (dk_hbm, dv_hbm)[part]
            remote(
                gsel.at[j, part], out.at[:, :, head_lanes(*target(j))],
                ret_send.at[part, j], ret_recv.at[part, j], at(c, *target(j)),
            ).wait_recv()

    for part, (stage, out) in enumerate(((att_st, att_hbm), (dq_st, dq_hbm))):
        for i in range(1, seq_count):
            q_copy(part, i).wait_send()
            came = lax.rem(z + seq_count - i, seq_count)
            remote(
                stage.at[came], out.at[:, group_lanes(lax.rem(z + i, seq_count))],
                out_send.at[part, i], out_recv.at[part, i], at(c, came, x),
            ).wait()
        own_out_copy(part).wait()
        own_ret_copy(part).wait()


def head_shards(queries, keys, values, q_gain, k_gain, gate, tile_count, tile_owner, visible, d_out):
    conv_count = lax.axis_size("conv")
    tensor_count = lax.axis_size("tensor")
    seq_count = lax.axis_size("seq")
    tiles, row_local, features = keys.shape
    size = q_gain.shape[0]
    count, width_all = queries.shape[1:]
    width = width_all // seq_count
    lanes = width_all // size * count
    bf, f32 = jnp.bfloat16, jnp.float32
    parts = seq_count * tensor_count
    far = conv_count // 2 - 1
    chunk = (2, tiles, row_local, size)
    rows = tiles * row_local
    v, dma = pltpu.VMEM, pltpu.SemaphoreType.DMA

    vmem = pl.BlockSpec(memory_space=pltpu.VMEM)
    smem = pl.BlockSpec(memory_space=pltpu.SMEM)
    hbm = pl.BlockSpec(memory_space=pl.ANY)
    att, dq, dk, dv = pl.pallas_call(
        partial(
            head_kernel, conv_count=conv_count, seq_count=seq_count, tensor_count=tensor_count
        ),
        out_shape=[jax.ShapeDtypeStruct((count, width_all), bf)] * 2
        + [jax.ShapeDtypeStruct(keys.shape, bf)] * 2,
        in_specs=[smem] * 3 + [vmem] * 3 + [hbm] * 4,
        out_specs=[hbm] * 4,
        scratch_shapes=[
            v((conv_count, parts) + chunk, bf),
            v((parts,) + chunk, bf),
            v((parts,) + chunk, bf),
            v((seq_count, count, width), bf),
            v((seq_count, count, width), bf),
            v((seq_count, 1, lanes // seq_count), jnp.int32),
            v((parts, rows, size), bf),
            v((parts, size, rows), bf),
            v((parts, size, rows), bf),
            v((parts, rows, lanes), bf),
            v((lanes, size), bf),
            v((size, lanes), bf),
            v((size, lanes), f32),
            v((size, lanes), f32),
            v((1, lanes), f32),
            v((size, lanes), bf),
            v((lanes, size), bf),
            v((1, lanes), f32),
            v((size, lanes), f32),
            v((rows, lanes), bf),
            v((seq_count, count, width), bf),
            v((seq_count, count, width), bf),
            v((conv_count, parts) + chunk, bf),
            v((parts,) + chunk, bf),
            dma((2, parts)), dma((far + 1, 2, parts)), dma((far + 1, 2, parts)),
            dma((far, parts)), dma((far, parts)), dma((parts,)), dma((parts,)),
            dma((2, seq_count)), dma((2, seq_count)), dma((2,)),
            dma((2, seq_count)), dma((2, seq_count)), dma((2,)),
            dma((far + 1, parts)), dma((far + 1, parts)), dma((far, parts)), dma((far, parts)),
            dma((2, parts)), dma((2, parts)), dma((2,)),
        ],
        compiler_params=pltpu.CompilerParams(
            collective_id=0, has_side_effects=True, vmem_limit_bytes=60 << 20
        ),
    )(
        tile_owner.T, tile_count, gate, visible, q_gain[None], k_gain[None],
        queries[0], d_out[0], keys, values,
    )
    return (att[None], dq[None], dk, dv)


def shards(queries, keys, *rest):
    heads = keys.shape[2] // rest[1].shape[0]
    seq_count, tensor_count = lax.axis_size("seq"), lax.axis_size("tensor")
    conv_count = lax.axis_size("conv")
    fits = heads == seq_count * tensor_count and conv_count % 2 == 0 and conv_count > 2
    fits = fits and keys.shape[1] % 16 == 0
    return (head_shards if fits else row_shards)(queries, keys, *rest)


def solution(mesh):
    in_specs = (
        P("conv", "seq", "tensor"),
        P("conv", ("seq", "tensor"), None),
        P("conv", ("seq", "tensor"), None),
        P(),
        P(),
        P(),
        P(),
        P(),
        P(),
        P("conv", "seq", "tensor"),
    )
    out_specs = (
        P("conv", "seq", "tensor"),
        P("conv", "seq", "tensor"),
        P("conv", ("seq", "tensor"), None),
        P("conv", ("seq", "tensor"), None),
    )
    return jax.shard_map(shards, mesh=mesh, in_specs=in_specs, out_specs=out_specs, check_vma=False)
```

```python
from functools import partial
import math

import jax
import jax.numpy as jnp
from jax import lax
from jax.experimental import pallas as pl
from jax.experimental.pallas import tpu as pltpu
from jax.sharding import PartitionSpec as P

TILE = 1601


EPSILON = 1e-05


def head_norm(inputs, norm_gain):
    mean_square = jnp.mean(inputs * inputs, axis=-1, keepdims=True)
    return inputs * lax.rsqrt(mean_square + EPSILON) * norm_gain


def key_mask(seen_tiles, tile_index, row_start, row_count):
    row_ids = row_start + jnp.arange(row_count, dtype=jnp.int32)
    return (seen_tiles > tile_index)[:, None] & (row_ids < TILE)[None, :]


def tile_weights(query_bf, key_tile, visible_keys, score_scale):
    scores = (
        jnp.einsum("pkgd,rkd->kgpr", query_bf, key_tile, preferred_element_type=jnp.float32)
        * score_scale
    )
    return jnp.where(visible_keys[None, None], jnp.exp(scores), 0.0)


def tile_forward(query_bf, key_tile, value_tile, visible_keys, score_scale):
    weights = tile_weights(query_bf, key_tile, visible_keys, score_scale)
    weighted = jnp.einsum(
        "kgpr,rkd->pkgd",
        weights.astype(jnp.bfloat16),
        value_tile,
        preferred_element_type=jnp.float32,
    )
    return (jnp.sum(weights, axis=-1), weighted)


def tile_gradients(
    query_bf,
    grad_bf,
    key_tile,
    value_tile,
    visible_keys,
    safe_sum,
    row_delta,
    score_scale,
    block_count,
):
    weights = tile_weights(query_bf, key_tile, visible_keys, score_scale)
    probability = weights / safe_sum[..., None]
    grad_prob = jnp.einsum(
        "pkgd,rkd->kgpr", grad_bf, value_tile, preferred_element_type=jnp.float32
    )
    grad_score = (probability * (grad_prob - row_delta[..., None])).astype(jnp.bfloat16)
    prob_bf = probability.astype(jnp.bfloat16)
    grad_query = (
        jnp.einsum("kgpr,rkd->pkgd", grad_score, key_tile, preferred_element_type=jnp.float32)
        * score_scale
    )
    kv_local, group_size, token_count, row_count = grad_score.shape
    head_size = query_bf.shape[-1]
    block_tokens = token_count // block_count
    score_blocks = grad_score.reshape(kv_local, group_size, block_count, block_tokens, row_count)
    prob_blocks = prob_bf.reshape(kv_local, group_size, block_count, block_tokens, row_count)
    query_blocks = query_bf.reshape(block_count, block_tokens, kv_local, group_size, head_size)
    grad_blocks = grad_bf.reshape(block_count, block_tokens, kv_local, group_size, head_size)
    key_part = (
        jnp.einsum(
            "kgbpr,bpkgd->brkd", score_blocks, query_blocks, preferred_element_type=jnp.float32
        )
        * score_scale
    )
    value_part = jnp.einsum(
        "kgbpr,bpkgd->brkd", prob_blocks, grad_blocks, preferred_element_type=jnp.float32
    )
    key_part = jnp.sum(
        lax.optimization_barrier(key_part.astype(jnp.bfloat16)).astype(jnp.float32), axis=0
    )
    value_part = jnp.sum(
        lax.optimization_barrier(value_part.astype(jnp.bfloat16)).astype(jnp.float32), axis=0
    )
    return (
        grad_query,
        key_part.reshape(row_count, kv_local * head_size),
        value_part.reshape(row_count, kv_local * head_size),
    )


def attend_forward(query_bf, tile_keys, tile_values, seen_tiles, row_start, score_scale):
    row_count, slot_count, features = tile_keys.shape
    token_count, kv_local, group_size, head_size = query_bf.shape
    weight_sum = jnp.zeros((kv_local, group_size, token_count), jnp.float32)
    weighted = jnp.zeros(query_bf.shape, jnp.float32)
    for tile_index in range(slot_count):
        key_tile = tile_keys[:, tile_index].reshape(row_count, kv_local, head_size)
        value_tile = tile_values[:, tile_index].reshape(row_count, kv_local, head_size)
        visible_keys = key_mask(seen_tiles, tile_index, row_start, row_count)
        work = partial(tile_forward, query_bf, key_tile, value_tile, visible_keys, score_scale)
        part_sum, part_weighted = work()
        weight_sum = weight_sum + part_sum
        weighted = weighted + part_weighted
    return (weight_sum, weighted)


def attend_backward(
    query_bf,
    grad_bf,
    tile_keys,
    tile_values,
    seen_tiles,
    row_start,
    safe_sum,
    row_delta,
    score_scale,
    block_tokens,
):
    row_count, slot_count, features = tile_keys.shape
    token_count, kv_local, group_size, head_size = query_bf.shape
    block_count = token_count // block_tokens
    grad_query = jnp.zeros(query_bf.shape, jnp.float32)
    key_parts = []
    value_parts = []
    for tile_index in range(slot_count):
        key_tile = tile_keys[:, tile_index].reshape(row_count, kv_local, head_size)
        value_tile = tile_values[:, tile_index].reshape(row_count, kv_local, head_size)
        visible_keys = key_mask(seen_tiles, tile_index, row_start, row_count)
        work = partial(
            tile_gradients,
            query_bf,
            grad_bf,
            key_tile,
            value_tile,
            visible_keys,
            safe_sum,
            row_delta,
            score_scale,
            block_count,
        )
        part_query, key_part, value_part = work()
        grad_query = grad_query + part_query
        key_parts.append(key_part)
        value_parts.append(value_part)
    return (grad_query, jnp.stack(key_parts, axis=1), jnp.stack(value_parts, axis=1))


def row_shards(queries, keys, values, q_gain, k_gain, gate, tile_count, tile_owner, visible, d_out):
    conv_count = lax.axis_size("conv")
    tensor_count = lax.axis_size("tensor")
    conv_index = lax.axis_index("conv")
    sequence_index = lax.axis_index("seq")
    slot_count, row_local, features = keys.shape
    head_size = q_gain.shape[0]
    kv_heads = features // head_size
    kv_local = kv_heads // tensor_count
    token_count = queries.shape[1]
    query_heads = queries.shape[2] // head_size
    group_size = query_heads // kv_local
    score_scale = 1.0 / math.sqrt(head_size)
    gate_value = jnp.tanh(gate[0])
    conv_ids = jnp.arange(conv_count, dtype=jnp.int32)
    transfers = (tile_owner == conv_index).astype(jnp.bfloat16)
    own_owners = lax.dynamic_index_in_dim(tile_owner, conv_index, 0, keepdims=False)
    takes = (own_owners[:, None] == conv_ids[None, :]).astype(jnp.bfloat16)
    own_count = lax.dynamic_index_in_dim(tile_count, conv_index, 0, keepdims=False)
    seen_all = jnp.minimum(
        lax.dynamic_index_in_dim(visible, conv_index, 0, keepdims=False), own_count
    )
    key_raw = keys.astype(jnp.float32).reshape(slot_count, row_local, kv_heads, head_size)
    key_normed, key_back = jax.vjp(lambda inputs: head_norm(inputs, k_gain), key_raw)
    key_halfprec = key_normed.astype(jnp.bfloat16).reshape(slot_count, row_local, features)
    outgoing_keys = jnp.einsum(
        "wn,nki->wki", transfers, key_halfprec, preferred_element_type=jnp.float32
    ).astype(jnp.bfloat16)
    send_values = jnp.einsum(
        "wn,nki->wki", transfers, values, preferred_element_type=jnp.float32
    ).astype(jnp.bfloat16)
    got_keys, got_values = (
        lax.all_to_all(
            lax.all_to_all(outgoing_keys, "conv", split_axis=0, concat_axis=0, tiled=True),
            "tensor",
            split_axis=2,
            concat_axis=1,
            tiled=True,
        ),
        lax.all_to_all(
            lax.all_to_all(send_values, "conv", split_axis=0, concat_axis=0, tiled=True),
            "tensor",
            split_axis=2,
            concat_axis=1,
            tiled=True,
        ),
    )
    tile_keys = jnp.einsum(
        "to,orf->rtf", takes, got_keys, preferred_element_type=jnp.float32
    ).astype(jnp.bfloat16)
    tile_values = jnp.einsum(
        "to,orf->rtf", takes, got_values, preferred_element_type=jnp.float32
    ).astype(jnp.bfloat16)
    query_raw = queries[0].astype(jnp.float32).reshape(token_count, query_heads, head_size)
    query_normed, query_back = jax.vjp(lambda inputs: head_norm(inputs, q_gain), query_raw)
    query_bf = query_normed.astype(jnp.bfloat16).reshape(
        token_count, kv_local, group_size, head_size
    )
    grad_bf = (
        (gate_value * d_out[0].astype(jnp.float32))
        .astype(jnp.bfloat16)
        .reshape(token_count, kv_local, group_size, head_size)
    )
    own_start = sequence_index * token_count
    all_queries = lax.all_gather(query_bf, "seq", axis=0, tiled=True)
    all_grads = lax.all_gather(grad_bf, "seq", axis=0, tiled=True)
    share_rows = tile_keys.shape[0]
    row_start = sequence_index * share_rows
    part_sum, part_weighted = attend_forward(
        all_queries, tile_keys, tile_values, seen_all, row_start, score_scale
    )
    all_weighted, all_weight_sum = (
        lax.psum(part_weighted.astype(jnp.bfloat16), "seq").astype(jnp.float32),
        lax.psum(part_sum.astype(jnp.bfloat16), "seq").astype(jnp.float32),
    )
    safe_all = jnp.where(all_weight_sum > 0, all_weight_sum, 1.0)
    context_all = all_weighted / jnp.transpose(safe_all, (2, 0, 1))[..., None]
    context = lax.dynamic_slice_in_dim(context_all, own_start, token_count, 0)
    row_delta = jnp.transpose(
        jnp.sum(all_grads.astype(jnp.float32) * context_all, axis=-1), (1, 2, 0)
    )
    grad_part, key_sums, value_sums = attend_backward(
        all_queries,
        all_grads,
        tile_keys,
        tile_values,
        seen_all,
        row_start,
        safe_all,
        row_delta,
        score_scale,
        token_count,
    )
    grad_query = lax.psum_scatter(
        grad_part.astype(jnp.bfloat16), "seq", scatter_dimension=0, tiled=True
    ).astype(jnp.float32)
    attended = (
        (gate_value * context).astype(jnp.bfloat16).reshape(1, token_count, query_heads * head_size)
    )
    key_round = key_sums.astype(jnp.bfloat16)
    value_round = value_sums.astype(jnp.bfloat16)
    back_keys = jnp.einsum(
        "to,rtf->orf", takes, key_round, preferred_element_type=jnp.float32
    ).astype(jnp.bfloat16)
    back_values = jnp.einsum(
        "to,rtf->orf", takes, value_round, preferred_element_type=jnp.float32
    ).astype(jnp.bfloat16)
    returned_keys, returned_values = (
        lax.all_to_all(
            lax.all_to_all(back_keys, "conv", split_axis=0, concat_axis=0, tiled=True),
            "tensor",
            split_axis=1,
            concat_axis=2,
            tiled=True,
        ),
        lax.all_to_all(
            lax.all_to_all(back_values, "conv", split_axis=0, concat_axis=0, tiled=True),
            "tensor",
            split_axis=1,
            concat_axis=2,
            tiled=True,
        ),
    )
    positioned_keys = jnp.einsum(
        "ew,eig->wig", transfers, returned_keys, preferred_element_type=jnp.float32
    )
    d_values = jnp.einsum(
        "ew,eig->wig", transfers, returned_values, preferred_element_type=jnp.float32
    ).astype(jnp.bfloat16)
    d_keys = key_back(positioned_keys.reshape(slot_count, row_local, kv_heads, head_size))[0]
    d_keys = d_keys.astype(jnp.bfloat16).reshape(slot_count, row_local, features)
    d_queries = query_back(grad_query.reshape(token_count, query_heads, head_size))[0]
    d_queries = d_queries.astype(jnp.bfloat16).reshape(1, token_count, query_heads * head_size)
    return (attended, d_queries, d_keys, d_values)


LOG2E = math.log2(math.e)


def inverse_rms(inputs):
    return lax.rsqrt(jnp.mean(inputs * inputs, axis=-1, keepdims=True) + EPSILON)


def norm_back(inputs, inv, gained):
    return inv * gained - inputs * (inv * inv * inv) * jnp.mean(
        inputs * gained, axis=-1, keepdims=True
    )


def dot(lhs, rhs):
    return jnp.dot(lhs, rhs, preferred_element_type=jnp.float32)


def head_kernel(
    owners, counts, gate, visible_hbm, q_gain_hbm, k_gain_hbm, q_hbm, do_hbm, k_hbm, v_hbm,
    att_hbm, dq_hbm, dk_hbm, dv_hbm,
    visible, q_gain_ref, k_gain_ref, small_sem, raw, sel, kvc, qa, da, seen, kn, kt, vt, wts, qs, qst, dt, acc, total, scaled_t, dos, delta,
    dqt, dss, att_st, dq_st, grads, gsel,
    own_sem, conv_send, conv_recv, relay_send, relay_recv, kv_send, kv_recv,
    q_send, q_recv, own_q_sem, out_send, out_recv, own_out_sem,
    back_send, back_recv, backrelay_send, backrelay_recv, ret_send, ret_recv, own_ret_sem,
    *, conv_count, seq_count, tensor_count,
):
    c = lax.axis_index("conv")
    z = lax.axis_index("seq")
    x = lax.axis_index("tensor")
    tiles, row_local, features = k_hbm.shape
    size = q_gain_ref.shape[1]
    count = q_hbm.shape[0]
    width = qa.shape[2]
    group = width // size
    lanes = group * count
    parts = seq_count * tensor_count
    rows = tiles * row_local
    heads_side = features // size // tensor_count
    scale = 1.0 / math.sqrt(size)

    def at(conv, seq, tensor):
        return {"conv": conv, "seq": seq, "tensor": tensor}

    def remote(src, dst, send, recv, device):
        return pltpu.make_async_remote_copy(
            src_ref=src, dst_ref=dst, send_sem=send, recv_sem=recv,
            device_id=device, device_id_type=pl.DeviceIdType.MESH,
        )

    def steps(j):
        return seq_count - 1 - j // tensor_count, tensor_count - 1 - j % tensor_count

    half = z // (seq_count // 2)

    def hop(q):
        k = 1 + (q + seq_count // 2 + seq_count - 3) % (seq_count - 1)
        k = (q + seq_count - 1) // seq_count * k
        return lax.rem(k + half * (seq_count - 2 * k), seq_count)

    def place(k, n):
        return (seq_count - 1 - k) * tensor_count + n % tensor_count

    def send_order(n):
        return place(hop(n // tensor_count), n)

    def back_order(n):
        n = lax.rem(n + tensor_count, parts)
        return place(lax.rem(seq_count - hop(n // tensor_count), seq_count), n)

    def target(j):
        k, e = steps(j)
        return lax.rem(z + k, seq_count), lax.rem(x + e, tensor_count)

    def source(j):
        k, e = steps(j)
        return lax.rem(z + seq_count - k, seq_count), lax.rem(x + tensor_count - e, tensor_count)

    def head_lanes(seq, tensor):
        return pl.ds(pl.multiple_of((tensor * heads_side + seq) * size, size), size)

    def block_lanes(b, start=0, length=lanes):
        return pl.ds(pl.multiple_of(b * lanes + start, size), length)

    def group_lanes(seq):
        return pl.ds(pl.multiple_of(seq * width, width), width)

    partner = c + 1 - 2 * lax.rem(c, 2)
    siblings = [lax.rem(c + 2 * m, conv_count) for m in range(1, conv_count // 2)]
    fars = [lax.rem(partner + 2 * m, conv_count) for m in range(1, conv_count // 2)]
    others = [partner] + siblings
    own = parts - 1

    barrier = pltpu.get_barrier_semaphore()
    peers = [at(c, *target(j)) for j in range(own)] + [at(other, z, x) for other in others]
    for peer in peers:
        pl.semaphore_signal(barrier, inc=1, device_id=peer, device_id_type=pl.DeviceIdType.MESH)
    pl.semaphore_wait(barrier, len(peers))

    token_pairs = ((q_hbm, qa), (do_hbm, da))
    stores = (k_hbm, v_hbm)

    def q_copy(part, i):
        store, into = token_pairs[part]
        to = lax.rem(z + seq_count - i, seq_count)
        return remote(
            store.at[:, group_lanes(to)], into.at[z],
            q_send.at[part, i], q_recv.at[part, i], at(c, to, x),
        )

    def own_q_copy(part):
        store, into = token_pairs[part]
        return pltpu.make_async_copy(store.at[:, group_lanes(z)], into.at[z], own_q_sem.at[part])

    @pl.loop(1, seq_count)
    def _(q):
        for part in range(2):
            q_copy(part, seq_count - hop(q)).start()

    def raw_copy(j, part, n):
        src = stores[part].at[:, :, head_lanes(*target(j))]
        return remote(
            src, raw.at[c, j, part],
            conv_send.at[n, part, j], conv_recv.at[n, part, j], at(others[n], z, x),
        )

    def own_copy(j, part):
        src = stores[part].at[:, :, head_lanes(*target(j))]
        return pltpu.make_async_copy(src, raw.at[c, j, part], own_sem.at[part, j])

    @pl.loop(0, parts)
    def _(step):
        j = send_order(step)
        for n in reversed(range(len(others))):
            for part in range(2):
                raw_copy(j, part, n).start()
        for part in range(2):
            own_copy(j, part).start()

    for part in range(2):
        own_q_copy(part).start()
    small = [
        pltpu.make_async_copy(src, dst, small_sem.at[n])
        for n, (src, dst) in enumerate(
            ((visible_hbm, visible), (q_gain_hbm, q_gain_ref), (k_gain_hbm, k_gain_ref))
        )
    ]
    for copy in small:
        copy.start()
    for copy in small:
        copy.wait()

    seen_all = jnp.minimum(visible[pl.ds(c, 1), :], counts[c])
    for b in range(seq_count):
        piece = seen_all[:, b * count:(b + 1) * count]
        seen[b] = jnp.concatenate([piece] * group, axis=1)
    acc[...] = jnp.zeros_like(acc)
    total[...] = jnp.zeros_like(total)
    dqt[...] = jnp.zeros_like(dqt)
    q_gain = q_gain_ref[...]
    k_gain = k_gain_ref[...]
    gate_value = jnp.tanh(jnp.full((1, size), gate[0], jnp.float32))[:, :1]

    def relay(ref, j, m, send, recv):
        other = siblings[m]
        return remote(ref.at[other, j], ref.at[other, j], send.at[m, j], recv.at[m, j], at(partner, z, x))

    def relayed(ref, j, m, send, recv):
        return remote(ref.at[fars[m], j], ref.at[fars[m], j], send.at[m, j], recv.at[m, j], at(partner, z, x))

    def kv_copy(j):
        return remote(sel.at[j], kvc.at[j], kv_send.at[j], kv_recv.at[j], at(c, *target(j)))

    def take_tokens(q):
        i = lax.rem(seq_count - hop(q), seq_count)
        block = lax.rem(z + i, seq_count)

        @pl.when(q == 0)
        def _():
            for part in range(2):
                own_q_copy(part).wait()

        @pl.when(q > 0)
        def _():
            for part, (store, into) in enumerate(token_pairs):
                remote(
                    store.at[:, group_lanes(z)], into.at[block],
                    q_send.at[part, i], q_recv.at[part, i], at(c, block, x),
                ).wait_recv()

        for g in range(group):
            piece = pl.ds(g * size, size)
            some = block_lanes(block, g * count, count)
            query = qa[block, :, piece].astype(jnp.float32)
            normed = query * inverse_rms(query) * (q_gain * (scale * LOG2E))
            qs[some, :] = normed.astype(jnp.bfloat16)
            qst[:, some] = normed.T.astype(jnp.bfloat16)
            dt[:, some] = (da[block, :, piece].astype(jnp.float32) * gate_value).T

    @pl.loop(0, parts)
    def _(step):
        j = send_order(step)
        for m, other in enumerate(siblings):
            came = len(siblings) - m
            for part in range(2):
                remote(
                    raw.at[other, j, part], raw.at[other, j, part],
                    conv_send.at[came, part, j], conv_recv.at[came, part, j], at(other, z, x),
                ).wait_recv()
            relay(raw, j, m, relay_send, relay_recv).start()
        for part in range(2):
            own_copy(j, part).wait()
            remote(
                raw.at[partner, j, part], raw.at[partner, j, part],
                conv_send.at[0, part, j], conv_recv.at[0, part, j], at(partner, z, x),
            ).wait_recv()
        for m in range(len(siblings)):
            relayed(raw, j, m, relay_send, relay_recv).wait_recv()
        for tile in range(tiles):
            for part in range(2):
                value = raw[0, j, part, tile]
                for conv in range(1, conv_count):
                    value = jnp.where(owners[tile, c] == conv, raw[conv, j, part, tile], value)
                sel[j, part, tile] = value

        @pl.when(j < own)
        def _():
            kv_copy(j).start()

        @pl.when(step >= parts - seq_count)
        def _():
            take_tokens(step - (parts - seq_count))

    kvc[own] = sel[own]

    @pl.loop(0, parts)
    def _(n):
        j = send_order(n)

        @pl.when(j < own)
        def _():
            kv_copy(j).wait_recv()

        key = kvc[j, 0].reshape(rows, size).astype(jnp.float32)
        normed = key * inverse_rms(key) * k_gain
        kn[j] = normed.astype(jnp.bfloat16)
        kt[j] = normed.T.astype(jnp.bfloat16)
        vt[j] = kvc[j, 1].reshape(rows, size).astype(jnp.float32).T.astype(jnp.bfloat16)
        from_seq, from_tensor = source(j)
        left = TILE - (from_seq * tensor_count + from_tensor) * row_local

        for b in range(seq_count):
            some = pl.ds(b * lanes, lanes)
            seen_row = seen[b]
            scores = dot(kn[j], qst[:, some])
            part_sum = jnp.zeros((1, lanes), jnp.float32)
            for tile in range(tiles):
                limit = jnp.where(seen_row > tile, left, 0)
                w = jnp.exp2(scores[tile * row_local:(tile + 1) * row_local])
                w = jnp.where(lax.broadcasted_iota(jnp.int32, w.shape, 0) < limit, w, 0.0)
                part_sum = part_sum + jnp.sum(w, axis=0, keepdims=True)
                wts[j, pl.ds(tile * row_local, row_local), some] = w.astype(jnp.bfloat16)
            total[:, some] += part_sum
        for b in range(seq_count):
            some = pl.ds(b * lanes, lanes)
            acc[:, some] += dot(vt[j], wts[j, :, some])

    def out_copy(part, i):
        stage, out = ((att_st, att_hbm), (dq_st, dq_hbm))[part]
        to = lax.rem(z + i, seq_count)
        return remote(
            stage.at[to], out.at[:, group_lanes(z)],
            out_send.at[part, i], out_recv.at[part, seq_count - i], at(c, to, x),
        )

    def own_out_copy(part):
        stage, out = ((att_st, att_hbm), (dq_st, dq_hbm))[part]
        return pltpu.make_async_copy(stage.at[z], out.at[:, group_lanes(z)], own_out_sem.at[part])

    @pl.loop(0, seq_count)
    def _(n):
        i = hop(lax.rem(n + 1, seq_count))
        b = lax.rem(z + i, seq_count)
        some = block_lanes(b)
        sums = total[:, some]
        inv = 1.0 / jnp.where(sums > 0, sums, 1.0)
        ctx = acc[:, some] * inv
        for g in range(group):
            att_st[b, :, pl.ds(g * size, size)] = (
                (gate_value * ctx[:, g * count:(g + 1) * count]).T.astype(jnp.bfloat16)
            )
        scaled = (dt[:, some] * inv).astype(jnp.bfloat16)
        scaled32 = scaled.astype(jnp.float32)
        scaled_t[:, some] = scaled
        delta[:, some] = jnp.sum(scaled32 * ctx, axis=0, keepdims=True)

        @pl.when(n < seq_count - 1)
        def _():
            out_copy(0, i).start()

        for g in range(group):
            dos[block_lanes(b, g * count, count), :] = (
                scaled32[:, g * count:(g + 1) * count].T.astype(jnp.bfloat16)
            )

    own_out_copy(0).start()

    def back_copy(j, n):
        return remote(
            grads.at[c, j], grads.at[c, j], back_send.at[n, j], back_recv.at[n, j],
            at(others[n], z, x),
        )

    def ret_copy(part, j):
        out = (dk_hbm, dv_hbm)[part]
        return remote(
            gsel.at[j, part], out.at[:, :, head_lanes(z, x)],
            ret_send.at[part, j], ret_recv.at[part, j], at(c, *source(j)),
        )

    def own_ret_copy(part):
        out = (dk_hbm, dv_hbm)[part]
        return pltpu.make_async_copy(
            gsel.at[own, part], out.at[:, :, head_lanes(z, x)], own_ret_sem.at[part]
        )

    def pass_back(n):
        j = back_order(n)
        for m, other in enumerate(siblings):
            came = len(siblings) - m
            remote(
                grads.at[other, j], grads.at[other, j], back_send.at[came, j],
                back_recv.at[came, j], at(other, z, x),
            ).wait_recv()
            relay(grads, j, m, backrelay_send, backrelay_recv).start()
        remote(
            grads.at[partner, j], grads.at[partner, j], back_send.at[0, j],
            back_recv.at[0, j], at(partner, z, x),
        ).wait_recv()
        for m in range(len(siblings)):
            relayed(grads, j, m, backrelay_send, backrelay_recv).wait_recv()
        for tile in range(tiles):
            for part in range(2):
                value = jnp.zeros((row_local, size), jnp.bfloat16)
                for conv in range(conv_count):
                    value = jnp.where(owners[tile, conv] == c, grads[conv, j, part, tile], value)
                gsel[j, part, tile] = value

        @pl.when(j < own)
        def _():
            for part in range(2):
                ret_copy(part, j).start()

    @pl.loop(0, parts)
    def _(n):
        j = back_order(n)
        value = kvc[j, 1].reshape(rows, size)
        for b in range(seq_count):
            some = pl.ds(b * lanes, lanes)
            dp = dot(value, scaled_t[:, some])
            score = wts[j, :, some].astype(jnp.float32) * (dp - delta[:, some])
            dss[:, some] = score.astype(jnp.bfloat16)
        dv = dot(wts[j], dos[...])
        dk = dot(dss[...], qs[...])
        for b in range(seq_count):
            some = pl.ds(b * lanes, lanes)
            dqt[:, some] += dot(kt[j], dss[:, some])

        key = kvc[j, 0].reshape(rows, size).astype(jnp.float32)
        grad = dk * (1.0 / LOG2E) * k_gain
        grad = norm_back(key, inverse_rms(key), grad).astype(jnp.bfloat16)
        grads[c, j, 0] = grad.reshape(tiles, row_local, size)
        grads[c, j, 1] = dv.astype(jnp.bfloat16).reshape(tiles, row_local, size)
        for m in reversed(range(len(others))):
            back_copy(j, m).start()

        late = n - parts // 2

        @pl.when((late >= 0) & (late % 2 == 0))
        def _():
            pass_back(late // 2)

    passed = (parts - parts // 2 + 1) // 2
    pass_back(passed)

    @pl.loop(0, seq_count)
    def _(n):
        i = hop(lax.rem(n + 1, seq_count))
        b = lax.rem(z + i, seq_count)
        for g in range(group):
            piece = pl.ds(g * size, size)
            query = qa[b, :, piece].astype(jnp.float32)
            grad = dqt[:, block_lanes(b, g * count, count)].T * (q_gain * scale)
            dq_st[b, :, piece] = norm_back(query, inverse_rms(query), grad).astype(jnp.bfloat16)

        @pl.when(n < seq_count - 1)
        def _():
            out_copy(1, i).start()

    own_out_copy(1).start()

    @pl.loop(passed + 1, parts)
    def _(n):
        pass_back(n)

    for part in range(2):
        own_ret_copy(part).start()

    @pl.loop(0, parts)
    def _(j):
        for n in range(len(others)):
            for part in range(2):
                raw_copy(j, part, n).wait_send()
            back_copy(j, n).wait_send()
        for m in range(len(siblings)):
            relay(raw, j, m, relay_send, relay_recv).wait_send()
            relay(grads, j, m, backrelay_send, backrelay_recv).wait_send()

    @pl.loop(0, own)
    def _(j):
        kv_copy(j).wait_send()
        for part in range(2):
            ret_copy(part, j).wait_send()
            out = (dk_hbm, dv_hbm)[part]
            remote(
                gsel.at[j, part], out.at[:, :, head_lanes(*target(j))],
                ret_send.at[part, j], ret_recv.at[part, j], at(c, *target(j)),
            ).wait_recv()

    for part, (stage, out) in enumerate(((att_st, att_hbm), (dq_st, dq_hbm))):
        for i in range(1, seq_count):
            q_copy(part, i).wait_send()
            came = lax.rem(z + seq_count - i, seq_count)
            remote(
                stage.at[came], out.at[:, group_lanes(lax.rem(z + i, seq_count))],
                out_send.at[part, i], out_recv.at[part, i], at(c, came, x),
            ).wait()
        own_out_copy(part).wait()
        own_ret_copy(part).wait()


def head_shards(queries, keys, values, q_gain, k_gain, gate, tile_count, tile_owner, visible, d_out):
    conv_count = lax.axis_size("conv")
    tensor_count = lax.axis_size("tensor")
    seq_count = lax.axis_size("seq")
    tiles, row_local, features = keys.shape
    size = q_gain.shape[0]
    count, width_all = queries.shape[1:]
    width = width_all // seq_count
    lanes = width_all // size * count
    bf, f32 = jnp.bfloat16, jnp.float32
    parts = seq_count * tensor_count
    far = conv_count // 2 - 1
    chunk = (2, tiles, row_local, size)
    rows = tiles * row_local
    v, dma = pltpu.VMEM, pltpu.SemaphoreType.DMA

    smem = pl.BlockSpec(memory_space=pltpu.SMEM)
    hbm = pl.BlockSpec(memory_space=pl.ANY)
    att, dq, dk, dv = pl.pallas_call(
        partial(
            head_kernel, conv_count=conv_count, seq_count=seq_count, tensor_count=tensor_count
        ),
        out_shape=[jax.ShapeDtypeStruct((count, width_all), bf)] * 2
        + [jax.ShapeDtypeStruct(keys.shape, bf)] * 2,
        in_specs=[smem] * 3 + [hbm] * 7,
        out_specs=[hbm] * 4,
        scratch_shapes=[
            v(visible.shape, jnp.int32),
            v((1, size), f32),
            v((1, size), f32),
            dma((3,)),
            v((conv_count, parts) + chunk, bf),
            v((parts,) + chunk, bf),
            v((parts,) + chunk, bf),
            v((seq_count, count, width), bf),
            v((seq_count, count, width), bf),
            v((seq_count, 1, lanes // seq_count), jnp.int32),
            v((parts, rows, size), bf),
            v((parts, size, rows), bf),
            v((parts, size, rows), bf),
            v((parts, rows, lanes), bf),
            v((lanes, size), bf),
            v((size, lanes), bf),
            v((size, lanes), f32),
            v((size, lanes), f32),
            v((1, lanes), f32),
            v((size, lanes), bf),
            v((lanes, size), bf),
            v((1, lanes), f32),
            v((size, lanes), f32),
            v((rows, lanes), bf),
            v((seq_count, count, width), bf),
            v((seq_count, count, width), bf),
            v((conv_count, parts) + chunk, bf),
            v((parts,) + chunk, bf),
            dma((2, parts)), dma((far + 1, 2, parts)), dma((far + 1, 2, parts)),
            dma((far, parts)), dma((far, parts)), dma((parts,)), dma((parts,)),
            dma((2, seq_count)), dma((2, seq_count)), dma((2,)),
            dma((2, seq_count)), dma((2, seq_count)), dma((2,)),
            dma((far + 1, parts)), dma((far + 1, parts)), dma((far, parts)), dma((far, parts)),
            dma((2, parts)), dma((2, parts)), dma((2,)),
        ],
        compiler_params=pltpu.CompilerParams(
            collective_id=0, has_side_effects=True, vmem_limit_bytes=48 << 20
        ),
    )(
        tile_owner.T, tile_count, gate,
        *[
            pltpu.with_memory_space_constraint(a, pltpu.HBM)
            for a in (
                visible, q_gain[None], k_gain[None], queries[0], d_out[0], keys, values,
            )
        ],
    )
    return store_results(att[None], dq[None], dk, dv)


def store_kernel(*refs):
    count = len(refs) // 2
    saves = [
        pltpu.make_async_copy(src, dst, refs[-1].at[n])
        for n, (src, dst) in enumerate(zip(refs[:count], refs[count:]))
    ]
    for save in saves:
        save.start()
    for save in saves:
        save.wait()


def store_results(*results):
    return pl.pallas_call(
        store_kernel,
        out_shape=[jax.ShapeDtypeStruct(r.shape, r.dtype) for r in results],
        in_specs=[pl.BlockSpec(memory_space=pltpu.VMEM)] * len(results),
        out_specs=[pl.BlockSpec(memory_space=pltpu.HBM)] * len(results),
        scratch_shapes=[pltpu.SemaphoreType.DMA((len(results),))],
        compiler_params=pltpu.CompilerParams(vmem_limit_bytes=8 << 20),
    )(*results)


def shards(queries, keys, *rest):
    heads = keys.shape[2] // rest[1].shape[0]
    seq_count, tensor_count = lax.axis_size("seq"), lax.axis_size("tensor")
    conv_count = lax.axis_size("conv")
    fits = heads == seq_count * tensor_count and conv_count % 2 == 0 and conv_count > 2
    fits = fits and keys.shape[1] % 16 == 0
    return (head_shards if fits else row_shards)(queries, keys, *rest)


def solution(mesh):
    in_specs = (
        P("conv", "seq", "tensor"),
        P("conv", ("seq", "tensor"), None),
        P("conv", ("seq", "tensor"), None),
        P(),
        P(),
        P(),
        P(),
        P(),
        P(),
        P("conv", "seq", "tensor"),
    )
    out_specs = (
        P("conv", "seq", "tensor"),
        P("conv", "seq", "tensor"),
        P("conv", ("seq", "tensor"), None),
        P("conv", ("seq", "tensor"), None),
    )
    return jax.shard_map(shards, mesh=mesh, in_specs=in_specs, out_specs=out_specs, check_vma=False)
```

```python
from functools import partial
import math

import jax
import jax.numpy as jnp
from jax import lax
from jax.experimental import pallas as pl
from jax.experimental.pallas import tpu as pltpu
from jax.sharding import PartitionSpec as P

TILE = 1601


EPSILON = 1e-05


def head_norm(inputs, norm_gain):
    mean_square = jnp.mean(inputs * inputs, axis=-1, keepdims=True)
    return inputs * lax.rsqrt(mean_square + EPSILON) * norm_gain


def key_mask(seen_tiles, tile_index, row_start, row_count):
    row_ids = row_start + jnp.arange(row_count, dtype=jnp.int32)
    return (seen_tiles > tile_index)[:, None] & (row_ids < TILE)[None, :]


def tile_weights(query_bf, key_tile, visible_keys, score_scale):
    scores = (
        jnp.einsum("pkgd,rkd->kgpr", query_bf, key_tile, preferred_element_type=jnp.float32)
        * score_scale
    )
    return jnp.where(visible_keys[None, None], jnp.exp(scores), 0.0)


def tile_forward(query_bf, key_tile, value_tile, visible_keys, score_scale):
    weights = tile_weights(query_bf, key_tile, visible_keys, score_scale)
    weighted = jnp.einsum(
        "kgpr,rkd->pkgd",
        weights.astype(jnp.bfloat16),
        value_tile,
        preferred_element_type=jnp.float32,
    )
    return (jnp.sum(weights, axis=-1), weighted)


def tile_gradients(
    query_bf,
    grad_bf,
    key_tile,
    value_tile,
    visible_keys,
    safe_sum,
    row_delta,
    score_scale,
    block_count,
):
    weights = tile_weights(query_bf, key_tile, visible_keys, score_scale)
    probability = weights / safe_sum[..., None]
    grad_prob = jnp.einsum(
        "pkgd,rkd->kgpr", grad_bf, value_tile, preferred_element_type=jnp.float32
    )
    grad_score = (probability * (grad_prob - row_delta[..., None])).astype(jnp.bfloat16)
    prob_bf = probability.astype(jnp.bfloat16)
    grad_query = (
        jnp.einsum("kgpr,rkd->pkgd", grad_score, key_tile, preferred_element_type=jnp.float32)
        * score_scale
    )
    kv_local, group_size, token_count, row_count = grad_score.shape
    head_size = query_bf.shape[-1]
    block_tokens = token_count // block_count
    score_blocks = grad_score.reshape(kv_local, group_size, block_count, block_tokens, row_count)
    prob_blocks = prob_bf.reshape(kv_local, group_size, block_count, block_tokens, row_count)
    query_blocks = query_bf.reshape(block_count, block_tokens, kv_local, group_size, head_size)
    grad_blocks = grad_bf.reshape(block_count, block_tokens, kv_local, group_size, head_size)
    key_part = (
        jnp.einsum(
            "kgbpr,bpkgd->brkd", score_blocks, query_blocks, preferred_element_type=jnp.float32
        )
        * score_scale
    )
    value_part = jnp.einsum(
        "kgbpr,bpkgd->brkd", prob_blocks, grad_blocks, preferred_element_type=jnp.float32
    )
    key_part = jnp.sum(
        lax.optimization_barrier(key_part.astype(jnp.bfloat16)).astype(jnp.float32), axis=0
    )
    value_part = jnp.sum(
        lax.optimization_barrier(value_part.astype(jnp.bfloat16)).astype(jnp.float32), axis=0
    )
    return (
        grad_query,
        key_part.reshape(row_count, kv_local * head_size),
        value_part.reshape(row_count, kv_local * head_size),
    )


def attend_forward(query_bf, tile_keys, tile_values, seen_tiles, row_start, score_scale):
    row_count, slot_count, features = tile_keys.shape
    token_count, kv_local, group_size, head_size = query_bf.shape
    weight_sum = jnp.zeros((kv_local, group_size, token_count), jnp.float32)
    weighted = jnp.zeros(query_bf.shape, jnp.float32)
    for tile_index in range(slot_count):
        key_tile = tile_keys[:, tile_index].reshape(row_count, kv_local, head_size)
        value_tile = tile_values[:, tile_index].reshape(row_count, kv_local, head_size)
        visible_keys = key_mask(seen_tiles, tile_index, row_start, row_count)
        work = partial(tile_forward, query_bf, key_tile, value_tile, visible_keys, score_scale)
        part_sum, part_weighted = work()
        weight_sum = weight_sum + part_sum
        weighted = weighted + part_weighted
    return (weight_sum, weighted)


def attend_backward(
    query_bf,
    grad_bf,
    tile_keys,
    tile_values,
    seen_tiles,
    row_start,
    safe_sum,
    row_delta,
    score_scale,
    block_tokens,
):
    row_count, slot_count, features = tile_keys.shape
    token_count, kv_local, group_size, head_size = query_bf.shape
    block_count = token_count // block_tokens
    grad_query = jnp.zeros(query_bf.shape, jnp.float32)
    key_parts = []
    value_parts = []
    for tile_index in range(slot_count):
        key_tile = tile_keys[:, tile_index].reshape(row_count, kv_local, head_size)
        value_tile = tile_values[:, tile_index].reshape(row_count, kv_local, head_size)
        visible_keys = key_mask(seen_tiles, tile_index, row_start, row_count)
        work = partial(
            tile_gradients,
            query_bf,
            grad_bf,
            key_tile,
            value_tile,
            visible_keys,
            safe_sum,
            row_delta,
            score_scale,
            block_count,
        )
        part_query, key_part, value_part = work()
        grad_query = grad_query + part_query
        key_parts.append(key_part)
        value_parts.append(value_part)
    return (grad_query, jnp.stack(key_parts, axis=1), jnp.stack(value_parts, axis=1))


def row_shards(queries, keys, values, q_gain, k_gain, gate, tile_count, tile_owner, visible, d_out):
    conv_count = lax.axis_size("conv")
    tensor_count = lax.axis_size("tensor")
    conv_index = lax.axis_index("conv")
    sequence_index = lax.axis_index("seq")
    slot_count, row_local, features = keys.shape
    head_size = q_gain.shape[0]
    kv_heads = features // head_size
    kv_local = kv_heads // tensor_count
    token_count = queries.shape[1]
    query_heads = queries.shape[2] // head_size
    group_size = query_heads // kv_local
    score_scale = 1.0 / math.sqrt(head_size)
    gate_value = jnp.tanh(gate[0])
    conv_ids = jnp.arange(conv_count, dtype=jnp.int32)
    transfers = (tile_owner == conv_index).astype(jnp.bfloat16)
    own_owners = lax.dynamic_index_in_dim(tile_owner, conv_index, 0, keepdims=False)
    takes = (own_owners[:, None] == conv_ids[None, :]).astype(jnp.bfloat16)
    own_count = lax.dynamic_index_in_dim(tile_count, conv_index, 0, keepdims=False)
    seen_all = jnp.minimum(
        lax.dynamic_index_in_dim(visible, conv_index, 0, keepdims=False), own_count
    )
    key_raw = keys.astype(jnp.float32).reshape(slot_count, row_local, kv_heads, head_size)
    key_normed, key_back = jax.vjp(lambda inputs: head_norm(inputs, k_gain), key_raw)
    key_halfprec = key_normed.astype(jnp.bfloat16).reshape(slot_count, row_local, features)
    outgoing_keys = jnp.einsum(
        "wn,nki->wki", transfers, key_halfprec, preferred_element_type=jnp.float32
    ).astype(jnp.bfloat16)
    send_values = jnp.einsum(
        "wn,nki->wki", transfers, values, preferred_element_type=jnp.float32
    ).astype(jnp.bfloat16)
    got_keys, got_values = (
        lax.all_to_all(
            lax.all_to_all(outgoing_keys, "conv", split_axis=0, concat_axis=0, tiled=True),
            "tensor",
            split_axis=2,
            concat_axis=1,
            tiled=True,
        ),
        lax.all_to_all(
            lax.all_to_all(send_values, "conv", split_axis=0, concat_axis=0, tiled=True),
            "tensor",
            split_axis=2,
            concat_axis=1,
            tiled=True,
        ),
    )
    tile_keys = jnp.einsum(
        "to,orf->rtf", takes, got_keys, preferred_element_type=jnp.float32
    ).astype(jnp.bfloat16)
    tile_values = jnp.einsum(
        "to,orf->rtf", takes, got_values, preferred_element_type=jnp.float32
    ).astype(jnp.bfloat16)
    query_raw = queries[0].astype(jnp.float32).reshape(token_count, query_heads, head_size)
    query_normed, query_back = jax.vjp(lambda inputs: head_norm(inputs, q_gain), query_raw)
    query_bf = query_normed.astype(jnp.bfloat16).reshape(
        token_count, kv_local, group_size, head_size
    )
    grad_bf = (
        (gate_value * d_out[0].astype(jnp.float32))
        .astype(jnp.bfloat16)
        .reshape(token_count, kv_local, group_size, head_size)
    )
    own_start = sequence_index * token_count
    all_queries = lax.all_gather(query_bf, "seq", axis=0, tiled=True)
    all_grads = lax.all_gather(grad_bf, "seq", axis=0, tiled=True)
    share_rows = tile_keys.shape[0]
    row_start = sequence_index * share_rows
    part_sum, part_weighted = attend_forward(
        all_queries, tile_keys, tile_values, seen_all, row_start, score_scale
    )
    all_weighted, all_weight_sum = (
        lax.psum(part_weighted.astype(jnp.bfloat16), "seq").astype(jnp.float32),
        lax.psum(part_sum.astype(jnp.bfloat16), "seq").astype(jnp.float32),
    )
    safe_all = jnp.where(all_weight_sum > 0, all_weight_sum, 1.0)
    context_all = all_weighted / jnp.transpose(safe_all, (2, 0, 1))[..., None]
    context = lax.dynamic_slice_in_dim(context_all, own_start, token_count, 0)
    row_delta = jnp.transpose(
        jnp.sum(all_grads.astype(jnp.float32) * context_all, axis=-1), (1, 2, 0)
    )
    grad_part, key_sums, value_sums = attend_backward(
        all_queries,
        all_grads,
        tile_keys,
        tile_values,
        seen_all,
        row_start,
        safe_all,
        row_delta,
        score_scale,
        token_count,
    )
    grad_query = lax.psum_scatter(
        grad_part.astype(jnp.bfloat16), "seq", scatter_dimension=0, tiled=True
    ).astype(jnp.float32)
    attended = (
        (gate_value * context).astype(jnp.bfloat16).reshape(1, token_count, query_heads * head_size)
    )
    key_round = key_sums.astype(jnp.bfloat16)
    value_round = value_sums.astype(jnp.bfloat16)
    back_keys = jnp.einsum(
        "to,rtf->orf", takes, key_round, preferred_element_type=jnp.float32
    ).astype(jnp.bfloat16)
    back_values = jnp.einsum(
        "to,rtf->orf", takes, value_round, preferred_element_type=jnp.float32
    ).astype(jnp.bfloat16)
    returned_keys, returned_values = (
        lax.all_to_all(
            lax.all_to_all(back_keys, "conv", split_axis=0, concat_axis=0, tiled=True),
            "tensor",
            split_axis=1,
            concat_axis=2,
            tiled=True,
        ),
        lax.all_to_all(
            lax.all_to_all(back_values, "conv", split_axis=0, concat_axis=0, tiled=True),
            "tensor",
            split_axis=1,
            concat_axis=2,
            tiled=True,
        ),
    )
    positioned_keys = jnp.einsum(
        "ew,eig->wig", transfers, returned_keys, preferred_element_type=jnp.float32
    )
    d_values = jnp.einsum(
        "ew,eig->wig", transfers, returned_values, preferred_element_type=jnp.float32
    ).astype(jnp.bfloat16)
    d_keys = key_back(positioned_keys.reshape(slot_count, row_local, kv_heads, head_size))[0]
    d_keys = d_keys.astype(jnp.bfloat16).reshape(slot_count, row_local, features)
    d_queries = query_back(grad_query.reshape(token_count, query_heads, head_size))[0]
    d_queries = d_queries.astype(jnp.bfloat16).reshape(1, token_count, query_heads * head_size)
    return (attended, d_queries, d_keys, d_values)


LOG2E = math.log2(math.e)


def inverse_rms(inputs):
    return lax.rsqrt(jnp.mean(inputs * inputs, axis=-1, keepdims=True) + EPSILON)


def norm_back(inputs, inv, gained):
    return inv * gained - inputs * (inv * inv * inv) * jnp.mean(
        inputs * gained, axis=-1, keepdims=True
    )


def dot(lhs, rhs):
    return jnp.dot(lhs, rhs, preferred_element_type=jnp.float32)


def head_kernel(
    owners, counts, gate, visible_hbm, q_gain_hbm, k_gain_hbm, q_hbm, do_hbm, k_hbm, v_hbm,
    att_hbm, dq_hbm, dk_hbm, dv_hbm,
    visible, q_gain_ref, k_gain_ref, small_sem, raw, sel, kvc, qa, da, seen, kn, kt, vt, wts, qs, qst, dt, acc, total, scaled_t, dos, delta,
    dqt, dss, att_st, dq_st, grads, gsel,
    own_sem, conv_send, conv_recv, relay_send, relay_recv, kv_send, kv_recv,
    q_send, q_recv, own_q_sem, out_send, out_recv, own_out_sem,
    back_send, back_recv, backrelay_send, backrelay_recv, ret_send, ret_recv, own_ret_sem,
    *, conv_count, seq_count, tensor_count,
):
    c = lax.axis_index("conv")
    z = lax.axis_index("seq")
    x = lax.axis_index("tensor")
    tiles, row_local, features = k_hbm.shape
    size = q_gain_ref.shape[1]
    count = q_hbm.shape[0]
    width = qa.shape[2]
    group = width // size
    lanes = group * count
    parts = seq_count * tensor_count
    rows = tiles * row_local
    heads_side = features // size // tensor_count
    scale = 1.0 / math.sqrt(size)

    def at(conv, seq, tensor):
        return {"conv": conv, "seq": seq, "tensor": tensor}

    def remote(src, dst, send, recv, device):
        return pltpu.make_async_remote_copy(
            src_ref=src, dst_ref=dst, send_sem=send, recv_sem=recv,
            device_id=device, device_id_type=pl.DeviceIdType.MESH,
        )

    def steps(j):
        return seq_count - 1 - j // tensor_count, tensor_count - 1 - j % tensor_count

    half = z // (seq_count // 2)

    def hop(q):
        k = 1 + (q + seq_count // 2 + seq_count - 3) % (seq_count - 1)
        k = (q + seq_count - 1) // seq_count * k
        return lax.rem(k + half * (seq_count - 2 * k), seq_count)

    def place(k, n):
        return (seq_count - 1 - k) * tensor_count + n % tensor_count

    def send_order(n):
        return place(hop(n // tensor_count), n)

    def back_order(n):
        n = lax.rem(n + tensor_count, parts)
        return place(lax.rem(seq_count - hop(n // tensor_count), seq_count), n)

    def target(j):
        k, e = steps(j)
        return lax.rem(z + k, seq_count), lax.rem(x + e, tensor_count)

    def source(j):
        k, e = steps(j)
        return lax.rem(z + seq_count - k, seq_count), lax.rem(x + tensor_count - e, tensor_count)

    def head_lanes(seq, tensor):
        return pl.ds(pl.multiple_of((tensor * heads_side + seq) * size, size), size)

    def block_lanes(b, start=0, length=lanes):
        return pl.ds(pl.multiple_of(b * lanes + start, size), length)

    def group_lanes(seq):
        return pl.ds(pl.multiple_of(seq * width, width), width)

    partner = c + 1 - 2 * lax.rem(c, 2)
    siblings = [lax.rem(c + 2 * m, conv_count) for m in range(1, conv_count // 2)]
    fars = [lax.rem(partner + 2 * m, conv_count) for m in range(1, conv_count // 2)]
    others = [partner] + siblings
    own = parts - 1

    barrier = pltpu.get_barrier_semaphore()
    peers = [at(c, *target(j)) for j in range(own)] + [at(other, z, x) for other in others]
    for peer in peers:
        pl.semaphore_signal(barrier, inc=1, device_id=peer, device_id_type=pl.DeviceIdType.MESH)
    pl.semaphore_wait(barrier, len(peers))

    token_pairs = ((q_hbm, qa), (do_hbm, da))
    stores = (k_hbm, v_hbm)

    def q_copy(part, i):
        store, into = token_pairs[part]
        to = lax.rem(z + seq_count - i, seq_count)
        return remote(
            store.at[:, group_lanes(to)], into.at[z],
            q_send.at[part, i], q_recv.at[part, i], at(c, to, x),
        )

    def own_q_copy(part):
        store, into = token_pairs[part]
        return pltpu.make_async_copy(store.at[:, group_lanes(z)], into.at[z], own_q_sem.at[part])

    @pl.loop(1, seq_count)
    def _(q):
        for part in range(2):
            q_copy(part, seq_count - hop(q)).start()

    def raw_copy(j, part, n):
        src = stores[part].at[:, :, head_lanes(*target(j))]
        return remote(
            src, raw.at[c, j, part],
            conv_send.at[n, part, j], conv_recv.at[n, part, j], at(others[n], z, x),
        )

    def own_copy(j, part):
        src = stores[part].at[:, :, head_lanes(*target(j))]
        return pltpu.make_async_copy(src, raw.at[c, j, part], own_sem.at[part, j])

    @pl.loop(0, parts)
    def _(step):
        j = send_order(step)
        for n in reversed(range(len(others))):
            for part in range(2):
                raw_copy(j, part, n).start()
        for part in range(2):
            own_copy(j, part).start()

    for part in range(2):
        own_q_copy(part).start()
    small = [
        pltpu.make_async_copy(src, dst, small_sem.at[n])
        for n, (src, dst) in enumerate(
            ((visible_hbm, visible), (q_gain_hbm, q_gain_ref), (k_gain_hbm, k_gain_ref))
        )
    ]
    for copy in small:
        copy.start()
    for copy in small:
        copy.wait()

    seen_all = jnp.minimum(visible[pl.ds(c, 1), :], counts[c])
    for b in range(seq_count):
        piece = seen_all[:, b * count:(b + 1) * count]
        seen[b] = jnp.concatenate([piece] * group, axis=1)
    acc[...] = jnp.zeros_like(acc)
    total[...] = jnp.zeros_like(total)
    dqt[...] = jnp.zeros_like(dqt)
    q_gain = q_gain_ref[...]
    k_gain = k_gain_ref[...]
    gate_value = jnp.tanh(jnp.full((1, size), gate[0], jnp.float32))[:, :1]

    def relay(ref, j, m, send, recv):
        other = siblings[m]
        return remote(ref.at[other, j], ref.at[other, j], send.at[m, j], recv.at[m, j], at(partner, z, x))

    def relayed(ref, j, m, send, recv):
        return remote(ref.at[fars[m], j], ref.at[fars[m], j], send.at[m, j], recv.at[m, j], at(partner, z, x))

    def kv_copy(j):
        return remote(sel.at[j], kvc.at[j], kv_send.at[j], kv_recv.at[j], at(c, *target(j)))

    def take_tokens(q):
        i = lax.rem(seq_count - hop(q), seq_count)
        block = lax.rem(z + i, seq_count)

        @pl.when(q == 0)
        def _():
            for part in range(2):
                own_q_copy(part).wait()

        @pl.when(q > 0)
        def _():
            for part, (store, into) in enumerate(token_pairs):
                remote(
                    store.at[:, group_lanes(z)], into.at[block],
                    q_send.at[part, i], q_recv.at[part, i], at(c, block, x),
                ).wait_recv()

        for g in range(group):
            piece = pl.ds(g * size, size)
            some = block_lanes(block, g * count, count)
            query = qa[block, :, piece].astype(jnp.float32)
            normed = query * inverse_rms(query) * (q_gain * (scale * LOG2E))
            qs[some, :] = normed.astype(jnp.bfloat16)
            qst[:, some] = normed.T.astype(jnp.bfloat16)
            dt[:, some] = (da[block, :, piece].astype(jnp.float32) * gate_value).T

    @pl.loop(0, parts)
    def _(step):
        j = send_order(step)
        for m, other in enumerate(siblings):
            came = len(siblings) - m
            for part in range(2):
                remote(
                    raw.at[other, j, part], raw.at[other, j, part],
                    conv_send.at[came, part, j], conv_recv.at[came, part, j], at(other, z, x),
                ).wait_recv()
            relay(raw, j, m, relay_send, relay_recv).start()
        for part in range(2):
            own_copy(j, part).wait()
            remote(
                raw.at[partner, j, part], raw.at[partner, j, part],
                conv_send.at[0, part, j], conv_recv.at[0, part, j], at(partner, z, x),
            ).wait_recv()
        for m in range(len(siblings)):
            relayed(raw, j, m, relay_send, relay_recv).wait_recv()
        for tile in range(tiles):
            for part in range(2):
                value = raw[0, j, part, tile]
                for conv in range(1, conv_count):
                    value = jnp.where(owners[tile, c] == conv, raw[conv, j, part, tile], value)
                sel[j, part, tile] = value

        @pl.when(j < own)
        def _():
            kv_copy(j).start()

        @pl.when(step >= parts - seq_count)
        def _():
            take_tokens(step - (parts - seq_count))

    kvc[own] = sel[own]

    @pl.loop(0, parts)
    def _(n):
        j = send_order(n)

        @pl.when(j < own)
        def _():
            kv_copy(j).wait_recv()

        key = kvc[j, 0].reshape(rows, size).astype(jnp.float32)
        normed = key * inverse_rms(key) * k_gain
        kn[j] = normed.astype(jnp.bfloat16)
        kt[j] = normed.T.astype(jnp.bfloat16)
        vt[j] = kvc[j, 1].reshape(rows, size).astype(jnp.float32).T.astype(jnp.bfloat16)
        from_seq, from_tensor = source(j)
        left = TILE - (from_seq * tensor_count + from_tensor) * row_local

        for b in range(seq_count):
            some = pl.ds(b * lanes, lanes)
            seen_row = seen[b]
            scores = dot(kn[j], qst[:, some])
            part_sum = jnp.zeros((1, lanes), jnp.float32)
            for tile in range(tiles):
                limit = jnp.where(seen_row > tile, left, 0)
                w = jnp.exp2(scores[tile * row_local:(tile + 1) * row_local])
                w = jnp.where(lax.broadcasted_iota(jnp.int32, w.shape, 0) < limit, w, 0.0)
                part_sum = part_sum + jnp.sum(w, axis=0, keepdims=True)
                wts[j, pl.ds(tile * row_local, row_local), some] = w.astype(jnp.bfloat16)
            total[:, some] += part_sum
        for b in range(seq_count):
            some = pl.ds(b * lanes, lanes)
            acc[:, some] += dot(vt[j], wts[j, :, some])

    def out_copy(part, i):
        stage, out = ((att_st, att_hbm), (dq_st, dq_hbm))[part]
        to = lax.rem(z + i, seq_count)
        return remote(
            stage.at[to], out.at[:, group_lanes(z)],
            out_send.at[part, i], out_recv.at[part, seq_count - i], at(c, to, x),
        )

    def own_out_copy(part):
        stage, out = ((att_st, att_hbm), (dq_st, dq_hbm))[part]
        return pltpu.make_async_copy(stage.at[z], out.at[:, group_lanes(z)], own_out_sem.at[part])

    @pl.loop(0, seq_count)
    def _(n):
        i = hop(lax.rem(n + 1, seq_count))
        b = lax.rem(z + i, seq_count)
        some = block_lanes(b)
        sums = total[:, some]
        inv = 1.0 / jnp.where(sums > 0, sums, 1.0)
        ctx = acc[:, some] * inv
        for g in range(group):
            att_st[b, :, pl.ds(g * size, size)] = (
                (gate_value * ctx[:, g * count:(g + 1) * count]).T.astype(jnp.bfloat16)
            )
        scaled = (dt[:, some] * inv).astype(jnp.bfloat16)
        scaled32 = scaled.astype(jnp.float32)
        scaled_t[:, some] = scaled
        delta[:, some] = jnp.sum(scaled32 * ctx, axis=0, keepdims=True)

        @pl.when(n < seq_count - 1)
        def _():
            out_copy(0, i).start()

        for g in range(group):
            dos[block_lanes(b, g * count, count), :] = (
                scaled32[:, g * count:(g + 1) * count].T.astype(jnp.bfloat16)
            )

    own_out_copy(0).start()

    def back_copy(j, n):
        return remote(
            grads.at[c, j], grads.at[c, j], back_send.at[n, j], back_recv.at[n, j],
            at(others[n], z, x),
        )

    def ret_copy(part, j):
        out = (dk_hbm, dv_hbm)[part]
        return remote(
            gsel.at[j, part], out.at[:, :, head_lanes(z, x)],
            ret_send.at[part, j], ret_recv.at[part, j], at(c, *source(j)),
        )

    def own_ret_copy(part):
        out = (dk_hbm, dv_hbm)[part]
        return pltpu.make_async_copy(
            gsel.at[own, part], out.at[:, :, head_lanes(z, x)], own_ret_sem.at[part]
        )

    def pass_back(n):
        j = back_order(n)
        for m, other in enumerate(siblings):
            came = len(siblings) - m
            remote(
                grads.at[other, j], grads.at[other, j], back_send.at[came, j],
                back_recv.at[came, j], at(other, z, x),
            ).wait_recv()
            relay(grads, j, m, backrelay_send, backrelay_recv).start()
        remote(
            grads.at[partner, j], grads.at[partner, j], back_send.at[0, j],
            back_recv.at[0, j], at(partner, z, x),
        ).wait_recv()
        for m in range(len(siblings)):
            relayed(grads, j, m, backrelay_send, backrelay_recv).wait_recv()
        for tile in range(tiles):
            for part in range(2):
                value = jnp.zeros((row_local, size), jnp.bfloat16)
                for conv in range(conv_count):
                    value = jnp.where(owners[tile, conv] == c, grads[conv, j, part, tile], value)
                gsel[j, part, tile] = value

        @pl.when(j < own)
        def _():
            for part in range(2):
                ret_copy(part, j).start()

    @pl.loop(0, parts)
    def _(n):
        j = back_order(n)
        value = kvc[j, 1].reshape(rows, size)
        for b in range(seq_count):
            some = pl.ds(b * lanes, lanes)
            dp = dot(value, scaled_t[:, some])
            score = wts[j, :, some].astype(jnp.float32) * (dp - delta[:, some])
            dss[:, some] = score.astype(jnp.bfloat16)
        dv = dot(wts[j], dos[...])
        dk = dot(dss[...], qs[...])
        for b in range(seq_count):
            some = pl.ds(b * lanes, lanes)
            dqt[:, some] += dot(kt[j], dss[:, some])

        key = kvc[j, 0].reshape(rows, size).astype(jnp.float32)
        grad = dk * (1.0 / LOG2E) * k_gain
        grad = norm_back(key, inverse_rms(key), grad).astype(jnp.bfloat16)
        grads[c, j, 0] = grad.reshape(tiles, row_local, size)
        grads[c, j, 1] = dv.astype(jnp.bfloat16).reshape(tiles, row_local, size)
        for m in reversed(range(len(others))):
            back_copy(j, m).start()

        late = n - parts // 2

        @pl.when(late == 0)
        def _():
            pass_back(0)

    passed = 1
    pass_back(passed)

    @pl.loop(0, seq_count)
    def _(n):
        i = hop(lax.rem(n + 1, seq_count))
        b = lax.rem(z + i, seq_count)
        for g in range(group):
            piece = pl.ds(g * size, size)
            query = qa[b, :, piece].astype(jnp.float32)
            grad = dqt[:, block_lanes(b, g * count, count)].T * (q_gain * scale)
            dq_st[b, :, piece] = norm_back(query, inverse_rms(query), grad).astype(jnp.bfloat16)

        @pl.when(n < seq_count - 1)
        def _():
            out_copy(1, i).start()

    own_out_copy(1).start()

    @pl.loop(passed + 1, parts)
    def _(n):
        pass_back(n)

    for part in range(2):
        own_ret_copy(part).start()

    @pl.loop(0, parts)
    def _(j):
        for n in range(len(others)):
            for part in range(2):
                raw_copy(j, part, n).wait_send()
            back_copy(j, n).wait_send()
        for m in range(len(siblings)):
            relay(raw, j, m, relay_send, relay_recv).wait_send()
            relay(grads, j, m, backrelay_send, backrelay_recv).wait_send()

    @pl.loop(0, own)
    def _(j):
        kv_copy(j).wait_send()
        for part in range(2):
            ret_copy(part, j).wait_send()
            out = (dk_hbm, dv_hbm)[part]
            remote(
                gsel.at[j, part], out.at[:, :, head_lanes(*target(j))],
                ret_send.at[part, j], ret_recv.at[part, j], at(c, *target(j)),
            ).wait_recv()

    for part, (stage, out) in enumerate(((att_st, att_hbm), (dq_st, dq_hbm))):
        for i in range(1, seq_count):
            q_copy(part, i).wait_send()
            came = lax.rem(z + seq_count - i, seq_count)
            remote(
                stage.at[came], out.at[:, group_lanes(lax.rem(z + i, seq_count))],
                out_send.at[part, i], out_recv.at[part, i], at(c, came, x),
            ).wait()
        own_out_copy(part).wait()
        own_ret_copy(part).wait()


def head_shards(queries, keys, values, q_gain, k_gain, gate, tile_count, tile_owner, visible, d_out):
    conv_count = lax.axis_size("conv")
    tensor_count = lax.axis_size("tensor")
    seq_count = lax.axis_size("seq")
    tiles, row_local, features = keys.shape
    size = q_gain.shape[0]
    count, width_all = queries.shape[1:]
    width = width_all // seq_count
    lanes = width_all // size * count
    bf, f32 = jnp.bfloat16, jnp.float32
    parts = seq_count * tensor_count
    far = conv_count // 2 - 1
    chunk = (2, tiles, row_local, size)
    rows = tiles * row_local
    v, dma = pltpu.VMEM, pltpu.SemaphoreType.DMA

    smem = pl.BlockSpec(memory_space=pltpu.SMEM)
    hbm = pl.BlockSpec(memory_space=pl.ANY)
    att, dq, dk, dv = pl.pallas_call(
        partial(
            head_kernel, conv_count=conv_count, seq_count=seq_count, tensor_count=tensor_count
        ),
        out_shape=[jax.ShapeDtypeStruct((count, width_all), bf)] * 2
        + [jax.ShapeDtypeStruct(keys.shape, bf)] * 2,
        in_specs=[smem] * 3 + [hbm] * 7,
        out_specs=[hbm] * 4,
        scratch_shapes=[
            v(visible.shape, jnp.int32),
            v((1, size), f32),
            v((1, size), f32),
            dma((3,)),
            v((conv_count, parts) + chunk, bf),
            v((parts,) + chunk, bf),
            v((parts,) + chunk, bf),
            v((seq_count, count, width), bf),
            v((seq_count, count, width), bf),
            v((seq_count, 1, lanes // seq_count), jnp.int32),
            v((parts, rows, size), bf),
            v((parts, size, rows), bf),
            v((parts, size, rows), bf),
            v((parts, rows, lanes), bf),
            v((lanes, size), bf),
            v((size, lanes), bf),
            v((size, lanes), f32),
            v((size, lanes), f32),
            v((1, lanes), f32),
            v((size, lanes), bf),
            v((lanes, size), bf),
            v((1, lanes), f32),
            v((size, lanes), f32),
            v((rows, lanes), bf),
            v((seq_count, count, width), bf),
            v((seq_count, count, width), bf),
            v((conv_count, parts) + chunk, bf),
            v((parts,) + chunk, bf),
            dma((2, parts)), dma((far + 1, 2, parts)), dma((far + 1, 2, parts)),
            dma((far, parts)), dma((far, parts)), dma((parts,)), dma((parts,)),
            dma((2, seq_count)), dma((2, seq_count)), dma((2,)),
            dma((2, seq_count)), dma((2, seq_count)), dma((2,)),
            dma((far + 1, parts)), dma((far + 1, parts)), dma((far, parts)), dma((far, parts)),
            dma((2, parts)), dma((2, parts)), dma((2,)),
        ],
        compiler_params=pltpu.CompilerParams(
            collective_id=0, has_side_effects=True, vmem_limit_bytes=48 << 20
        ),
    )(
        tile_owner.T, tile_count, gate,
        *[
            pltpu.with_memory_space_constraint(a, pltpu.HBM)
            for a in (
                visible, q_gain[None], k_gain[None], queries[0], d_out[0], keys, values,
            )
        ],
    )
    return store_results(att[None], dq[None], dk, dv)


def store_kernel(*refs):
    count = len(refs) // 2
    saves = [
        pltpu.make_async_copy(src, dst, refs[-1].at[n])
        for n, (src, dst) in enumerate(zip(refs[:count], refs[count:]))
    ]
    for save in saves:
        save.start()
    for save in saves:
        save.wait()


def store_results(*results):
    return pl.pallas_call(
        store_kernel,
        out_shape=[jax.ShapeDtypeStruct(r.shape, r.dtype) for r in results],
        in_specs=[pl.BlockSpec(memory_space=pltpu.VMEM)] * len(results),
        out_specs=[pl.BlockSpec(memory_space=pltpu.HBM)] * len(results),
        scratch_shapes=[pltpu.SemaphoreType.DMA((len(results),))],
        compiler_params=pltpu.CompilerParams(vmem_limit_bytes=8 << 20),
    )(*results)


def shards(queries, keys, *rest):
    heads = keys.shape[2] // rest[1].shape[0]
    seq_count, tensor_count = lax.axis_size("seq"), lax.axis_size("tensor")
    conv_count = lax.axis_size("conv")
    fits = heads == seq_count * tensor_count and conv_count % 2 == 0 and conv_count > 2
    fits = fits and keys.shape[1] % 16 == 0
    return (head_shards if fits else row_shards)(queries, keys, *rest)


def solution(mesh):
    in_specs = (
        P("conv", "seq", "tensor"),
        P("conv", ("seq", "tensor"), None),
        P("conv", ("seq", "tensor"), None),
        P(),
        P(),
        P(),
        P(),
        P(),
        P(),
        P("conv", "seq", "tensor"),
    )
    out_specs = (
        P("conv", "seq", "tensor"),
        P("conv", "seq", "tensor"),
        P("conv", ("seq", "tensor"), None),
        P("conv", ("seq", "tensor"), None),
    )
    return jax.shard_map(shards, mesh=mesh, in_specs=in_specs, out_specs=out_specs, check_vma=False)
```
